8 devices in a mesh: dp: 1 (over z), cp: 8 (over y, x, core).
Axes of the slice: x: 2, y: 2, z: 1, core: 2. Of those that a mesh axis runs over, the one named last changes fastest.
Arguments:
- x_in: bfloat16 [8192, 3584], P(('dp', 'cp'))
- dy_in: bfloat16 [8192, 3584], P(('dp', 'cp'))
- doc_id: int32 [8192], P(('dp', 'cp'))
- w_q: bfloat16 [3584, 2, 256], replicated
- w_k: bfloat16 [3584, 1, 256], replicated
- w_v: bfloat16 [3584, 1, 256], replicated
- w_o: bfloat16 [2, 256, 3584], replicated
Outputs:
- output 1: bfloat16 [8192, 3584], P(('dp', 'cp'))
- output 2: bfloat16 [8192, 3584], P(('dp', 'cp'))
All inputs are finite; a program needn't handle non-finite values.
Results may differ from the reference program's by a relative error of at most 0.00929256.
Values are sent between devices in bfloat16 or wider.
A program may use at most 1 GiB of HBM per device.

```python
import jax
import jax.numpy as jnp
from jax import lax

D_MODEL = 3584
Q_HEADS = 2
KV_HEADS = 1
HEAD_DIM = 256
TOK_DEV = 1024
GROUP_DEVS = 8
SEQ_LEN = GROUP_DEVS * TOK_DEV
PIECE_LEN = TOK_DEV // 2
QUERY_GROUP = Q_HEADS // KV_HEADS
DOC_CUTS = max(1, GROUP_DEVS // 2)
NEG_BIG = -1.0e30


def stored_positions():
    row_idx = jnp.arange(SEQ_LEN, dtype=jnp.int32)
    owner_dev = row_idx // TOK_DEV
    offset = row_idx % TOK_DEV
    piece_idx = jnp.where(offset < PIECE_LEN, owner_dev, 2 * GROUP_DEVS - 1 - owner_dev)
    return piece_idx * PIECE_LEN + offset % PIECE_LEN


def setup_inputs(seed: int = 0, part: int = 0) -> dict:
    part_key = jax.random.fold_in(jax.random.key(seed), part)
    key_x, key_dy, key_doc = jax.random.split(part_key, 3)
    key_q, key_k, key_v, key_o = jax.random.split(jax.random.key(seed + 1), 4)
    in_scale = D_MODEL ** -0.5
    out_scale = (Q_HEADS * HEAD_DIM) ** -0.5
    x_in = jax.random.normal(key_x, (SEQ_LEN, D_MODEL), jnp.float32).astype(jnp.bfloat16)
    dy_in = jax.random.normal(key_dy, (SEQ_LEN, D_MODEL), jnp.float32).astype(jnp.bfloat16)
    cut_pos = jax.random.randint(key_doc, (DOC_CUTS,), 1, SEQ_LEN, dtype=jnp.int32)
    doc_id = jnp.sum((stored_positions()[:, None] >= cut_pos[None, :]).astype(jnp.int32), axis=1)
    w_q = (jax.random.normal(key_q, (D_MODEL, Q_HEADS, HEAD_DIM), jnp.float32) * in_scale).astype(jnp.bfloat16)
    w_k = (jax.random.normal(key_k, (D_MODEL, KV_HEADS, HEAD_DIM), jnp.float32) * in_scale).astype(jnp.bfloat16)
    w_v = (jax.random.normal(key_v, (D_MODEL, KV_HEADS, HEAD_DIM), jnp.float32) * in_scale).astype(jnp.bfloat16)
    w_o = (jax.random.normal(key_o, (Q_HEADS, HEAD_DIM, D_MODEL), jnp.float32) * out_scale).astype(jnp.bfloat16)
    return {'x_in': x_in, 'dy_in': dy_in, 'doc_id': doc_id, 'w_q': w_q, 'w_k': w_k, 'w_v': w_v, 'w_o': w_o}


def reference(x_in, dy_in, doc_id, w_q, w_k, w_v, w_o):
    score_scale = HEAD_DIM ** -0.5
    all_pos = stored_positions()
    wq_flat = w_q.reshape(D_MODEL, Q_HEADS * HEAD_DIM)
    wk_flat = w_k.reshape(D_MODEL, KV_HEADS * HEAD_DIM)
    wv_flat = w_v.reshape(D_MODEL, KV_HEADS * HEAD_DIM)
    wo_flat = w_o.reshape(Q_HEADS * HEAD_DIM, D_MODEL)
    q_all = jnp.dot(x_in, wq_flat, preferred_element_type=jnp.float32).astype(jnp.bfloat16)
    q_all = q_all.reshape(SEQ_LEN, KV_HEADS, QUERY_GROUP, HEAD_DIM)
    k_all = jnp.dot(x_in, wk_flat, preferred_element_type=jnp.float32).astype(jnp.bfloat16)
    v_all = jnp.dot(x_in, wv_flat, preferred_element_type=jnp.float32).astype(jnp.bfloat16)
    k_wide = k_all.reshape(SEQ_LEN, KV_HEADS, HEAD_DIM).astype(jnp.float32)
    v_wide = v_all.reshape(SEQ_LEN, KV_HEADS, HEAD_DIM).astype(jnp.float32)
    do_all = jnp.dot(dy_in, wo_flat.T, preferred_element_type=jnp.float32).astype(jnp.bfloat16)
    do_all = do_all.reshape(SEQ_LEN, KV_HEADS, QUERY_GROUP, HEAD_DIM)

    def block_step(grad_acc, block_idx):
        dk_acc, dv_acc = grad_acc
        row_start = block_idx * TOK_DEV
        q_blk = lax.dynamic_slice_in_dim(q_all, row_start, TOK_DEV, 0).astype(jnp.float32)
        do_blk = lax.dynamic_slice_in_dim(do_all, row_start, TOK_DEV, 0).astype(jnp.float32)
        pos_blk = lax.dynamic_slice_in_dim(all_pos, row_start, TOK_DEV, 0)
        doc_blk = lax.dynamic_slice_in_dim(doc_id, row_start, TOK_DEV, 0)
        visible = (all_pos[None, :] <= pos_blk[:, None]) & (doc_id[None, :] == doc_blk[:, None])
        scores = jnp.einsum('tkge,ske->tkgs', q_blk, k_wide) * score_scale
        scores = jnp.where(visible[:, None, None, :], scores, NEG_BIG)
        log_norm = jax.nn.logsumexp(scores, axis=-1, keepdims=True)
        prob_blk = jnp.exp(scores - log_norm).astype(jnp.bfloat16).astype(jnp.float32)
        out_blk = jnp.einsum('tkgs,ske->tkge', prob_blk, v_wide).astype(jnp.bfloat16).astype(jnp.float32)
        delta_row = jnp.sum(do_blk * out_blk, axis=-1, keepdims=True)
        d_prob = jnp.einsum('tkge,ske->tkgs', do_blk, v_wide)
        d_score = (prob_blk * (d_prob - delta_row)).astype(jnp.bfloat16).astype(jnp.float32)
        dq_blk = (jnp.einsum('tkgs,ske->tkge', d_score, k_wide) * score_scale).astype(jnp.bfloat16)
        dk_acc = dk_acc + jnp.einsum('tkgs,tkge->ske', d_score, q_blk) * score_scale
        dv_acc = dv_acc + jnp.einsum('tkgs,tkge->ske', prob_blk, do_blk)
        return (dk_acc, dv_acc), (out_blk.astype(jnp.bfloat16), dq_blk)

    zero_grad = jnp.zeros((SEQ_LEN, KV_HEADS, HEAD_DIM), jnp.float32)
    grad_sums, block_outs = lax.scan(block_step, (zero_grad, zero_grad), jnp.arange(GROUP_DEVS))
    dk_sum, dv_sum = grad_sums
    out_blocks, dq_blocks = block_outs
    out_all = out_blocks.reshape(SEQ_LEN, Q_HEADS * HEAD_DIM)
    dq_all = dq_blocks.reshape(SEQ_LEN, Q_HEADS * HEAD_DIM)
    y_out = jnp.dot(out_all, wo_flat, preferred_element_type=jnp.float32).astype(jnp.bfloat16)
    dk_bf = dk_sum.astype(jnp.bfloat16).reshape(SEQ_LEN, KV_HEADS * HEAD_DIM)
    dv_bf = dv_sum.astype(jnp.bfloat16).reshape(SEQ_LEN, KV_HEADS * HEAD_DIM)
    dx_wide = (jnp.dot(dq_all, wq_flat.T, preferred_element_type=jnp.float32)
               + jnp.dot(dk_bf, wk_flat.T, preferred_element_type=jnp.float32)
               + jnp.dot(dv_bf, wv_flat.T, preferred_element_type=jnp.float32))
    dx_out = dx_wide.astype(jnp.bfloat16)
    return y_out, dx_out
```

```python
import functools
import math

import jax
import jax.numpy as jnp
from jax import lax
from jax.experimental import pallas as pl
from jax.experimental.pallas import tpu as pltpu
from jax.sharding import PartitionSpec as P

NEG_BIG = -1.0e30
BF16 = jnp.bfloat16
F32 = jnp.float32
PIECE = 512
QT = 256
NT = (((1,), (1,)), ((), ()))
NN = (((1,), (0,)), ((), ()))
VMEM_LIMIT = 60 * 1024 * 1024


def dot(a, b, dims):
    return lax.dot_general(a, b, dims, preferred_element_type=F32)


def doc_start(bounds, pos):
    out = jnp.zeros_like(pos)
    for b in bounds:
        out = jnp.maximum(out, jnp.where(b <= pos, b, 0))
    return out


def doc_end(bounds, pos, seq_len):
    out = seq_len
    for b in bounds:
        out = jnp.minimum(out, jnp.where(b > pos, b, seq_len))
    return out


def owner_of(piece, n_dev):
    late = piece >= n_dev
    dev = jnp.where(late, 2 * n_dev - 1 - piece, piece)
    return dev, jnp.where(late, PIECE, 0)


def kv_proj_kernel(x_ref, wk_ref, wv_ref, kv_ref):
    x = x_ref[...]
    hd = wk_ref.shape[1]
    kv_ref[:, :hd] = dot(x, wk_ref[...], NN).astype(BF16)
    kv_ref[:, hd:] = dot(x, wv_ref[...], NN).astype(BF16)


def kv_proj(x, wk, wv):
    rows, d = x.shape
    hd = wk.shape[1]
    return pl.pallas_call(
        kv_proj_kernel,
        grid=(rows // 256,),
        in_specs=[
            pl.BlockSpec((256, d), lambda i: (i, 0)),
            pl.BlockSpec((d, hd), lambda i: (0, 0)),
            pl.BlockSpec((d, hd), lambda i: (0, 0)),
        ],
        out_specs=pl.BlockSpec((256, 2 * hd), lambda i: (i, 0)),
        out_shape=jax.ShapeDtypeStruct((rows, 2 * hd), BF16),
        compiler_params=pltpu.CompilerParams(vmem_limit_bytes=VMEM_LIMIT),
        cost_estimate=pl.CostEstimate(flops=2 * rows * d * 2 * hd, bytes_accessed=2 * rows * d, transcendentals=0),
        name="kv_proj",
    )(x, wk, wv)


def attn_q_kernel(n_dev, scale, sc_ref, q_ref, do_ref, kv_hbm, o_ref, dq_ref, ld_ref, kv_s, s_ref, mx_ref, l_ref, acc_ref, sem):
    t = pl.program_id(0)
    me = sc_ref[0]
    bounds = [sc_ref[1 + d] for d in range(4)]
    hd = acc_ref.shape[1]
    c2 = scale * math.log2(math.e)
    lo_e = doc_start(bounds, me * PIECE) // PIECE
    late = 2 * n_dev - 1 - me
    lo_l = doc_start(bounds, late * PIECE) // PIECE

    def each_piece(fn):
        for p in range(2 * n_dev):
            dev, off = (p, 0) if p < n_dev else (2 * n_dev - 1 - p, PIECE)
            need = ((p >= lo_e) & (p <= me)) | ((p >= lo_l) & (p <= late))

            @pl.when(need)
            def _():
                fn(pltpu.make_async_copy(kv_hbm.at[pl.ds(dev * 2 * PIECE + off, PIECE)], kv_s.at[p], sem))

    @pl.when(t == 0)
    def _():
        each_piece(lambda cp: cp.start())
        each_piece(lambda cp: cp.wait())

    piece = jnp.where(t < 2, me, late)
    q0 = piece * PIECE + (t % 2) * QT
    kt0 = doc_start(bounds, q0) // PIECE
    kt1 = piece + 1
    q2 = jnp.concatenate([q_ref[:, :hd], q_ref[:, hd:]], axis=0)
    do2 = jnp.concatenate([do_ref[:, :hd], do_ref[:, hd:]], axis=0)
    rpos = q0 + lax.broadcasted_iota(jnp.int32, (2 * QT, 1), 0) % QT
    rstart = doc_start(bounds, rpos)
    mx_ref[...] = jnp.full(mx_ref.shape, NEG_BIG, F32)

    @pl.loop(kt0, kt1)
    def _(kt):
        s = dot(q2, kv_s[kt, :, :hd], NT) * c2
        kpos = kt * PIECE + lax.broadcasted_iota(jnp.int32, (1, PIECE), 1)
        s = jnp.where((kpos <= rpos) & (kpos >= rstart), s, NEG_BIG)
        s_ref[kt] = s
        mx = mx_ref[...]
        for j in range(PIECE // 128):
            mx = jnp.maximum(mx, s[:, j * 128:(j + 1) * 128])
        mx_ref[...] = mx

    m = jnp.max(mx_ref[...], axis=1, keepdims=True)
    l_ref[...] = jnp.zeros(l_ref.shape, F32)
    acc_ref[...] = jnp.zeros(acc_ref.shape, F32)

    @pl.loop(kt0, kt1)
    def _(kt):
        p = jnp.exp2(s_ref[kt] - m)
        s_ref[kt] = p
        ls = l_ref[...]
        for j in range(PIECE // 128):
            ls = ls + p[:, j * 128:(j + 1) * 128]
        l_ref[...] = ls
        acc_ref[...] += dot(p.astype(BF16), kv_s[kt, :, hd:], NN)

    l = jnp.sum(l_ref[...], axis=1, keepdims=True)
    rl = 1.0 / l
    o2 = (acc_ref[...] * rl).astype(BF16)
    o_ref[:, :hd] = o2[:QT]
    o_ref[:, hd:] = o2[QT:]
    delta = jnp.sum(do2.astype(F32) * o2.astype(F32), axis=1, keepdims=True)
    l2 = m + jnp.log2(l)
    ld_ref[0, 0:1] = jnp.transpose(jnp.broadcast_to(l2, (2 * QT, 128)))[0:1]
    ld_ref[0, 1:2] = jnp.transpose(jnp.broadcast_to(delta, (2 * QT, 128)))[0:1]
    acc_ref[...] = jnp.zeros(acc_ref.shape, F32)

    @pl.loop(kt0, kt1)
    def _(kt):
        p = (s_ref[kt] * rl).astype(BF16).astype(F32)
        dp = dot(do2, kv_s[kt, :, hd:], NT)
        ds = (p * (dp - delta)).astype(BF16)
        acc_ref[...] += dot(ds, kv_s[kt, :, :hd], NN)

    dq2 = (acc_ref[...] * scale).astype(BF16)
    dq_ref[:, :hd] = dq2[:QT]
    dq_ref[:, hd:] = dq2[QT:]


def attn_q(sc, q, do, kv_all, n_dev, scale):
    rows, qd = q.shape
    hd = kv_all.shape[1] // 2
    blk = pl.BlockSpec((QT, qd), lambda t, sc: (t, 0))
    work = 4 * 2 * rows * qd * rows * n_dev // 2
    return pl.pallas_call(
        functools.partial(attn_q_kernel, n_dev, scale),
        grid_spec=pltpu.PrefetchScalarGridSpec(
            num_scalar_prefetch=1,
            grid=(rows // QT,),
            in_specs=[blk, blk, pl.BlockSpec(memory_space=pl.ANY)],
            out_specs=[blk, blk, pl.BlockSpec((1, 2, 2 * QT), lambda t, sc: (t, 0, 0))],
            scratch_shapes=[
                pltpu.VMEM((2 * n_dev, PIECE, 2 * hd), BF16),
                pltpu.VMEM((2 * n_dev, 2 * QT, PIECE), F32),
                pltpu.VMEM((2 * QT, 128), F32),
                pltpu.VMEM((2 * QT, 128), F32),
                pltpu.VMEM((2 * QT, hd), F32),
                pltpu.SemaphoreType.DMA,
            ],
        ),
        out_shape=[
            jax.ShapeDtypeStruct((rows, qd), BF16),
            jax.ShapeDtypeStruct((rows, qd), BF16),
            jax.ShapeDtypeStruct((rows // QT, 2, 2 * QT), F32),
        ],
        compiler_params=pltpu.CompilerParams(vmem_limit_bytes=VMEM_LIMIT, dimension_semantics=("arbitrary",)),
        cost_estimate=pl.CostEstimate(flops=work, bytes_accessed=16 * rows * qd, transcendentals=0),
        name="attn_q",
    )(sc, q, do, kv_all)


def attn_kv_kernel(n_dev, scale, sc_ref, kv_ref, ld_ref, qd_hbm, dkv_ref, qd_s, dk_ref, dv_ref, sem):
    g = pl.program_id(0)
    me = sc_ref[0]
    bounds = [sc_ref[1 + d] for d in range(4)]
    hd = dk_ref.shape[1]
    seq_len = 2 * n_dev * PIECE
    c2 = scale * math.log2(math.e)
    late = 2 * n_dev - 1 - me
    end_e = doc_end(bounds, me * PIECE + PIECE - 1, seq_len)
    end_l = doc_end(bounds, late * PIECE + PIECE - 1, seq_len)

    def each_piece(fn):
        for p in range(2 * n_dev):
            dev, off = (p, 0) if p < n_dev else (2 * n_dev - 1 - p, PIECE)
            need = ((p >= me) & (p * PIECE < end_e)) | ((p >= late) & (p * PIECE < end_l))

            @pl.when(need)
            def _():
                fn(pltpu.make_async_copy(qd_hbm.at[pl.ds(dev * 2 * PIECE + off, PIECE)], qd_s.at[p], sem))

    @pl.when(g == 0)
    def _():
        each_piece(lambda cp: cp.start())
        each_piece(lambda cp: cp.wait())

    kp = jnp.where(g == 0, me, late)
    end = jnp.where(g == 0, end_e, end_l)
    k = kv_ref[:, :hd]
    v = kv_ref[:, hd:]
    kpos = kp * PIECE + lax.broadcasted_iota(jnp.int32, (PIECE, 1), 0)
    dk_ref[...] = jnp.zeros(dk_ref.shape, F32)
    dv_ref[...] = jnp.zeros(dv_ref.shape, F32)

    @pl.loop(2 * kp, (end + QT - 1) // QT)
    def _(qt):
        qp = qt // 2
        half = qt % 2
        dev, off = owner_of(qp, n_dev)
        tile = dev * 4 + off // QT + half
        rows = pl.ds(pl.multiple_of(half * QT, QT), QT)
        q2 = jnp.concatenate([qd_s[qp, rows, 0:hd], qd_s[qp, rows, hd:2 * hd]], axis=0)
        do2 = jnp.concatenate([qd_s[qp, rows, 2 * hd:3 * hd], qd_s[qp, rows, 3 * hd:4 * hd]], axis=0)
        l2 = ld_ref[tile, 0:1, :]
        delta = ld_ref[tile, 1:2, :]
        qpos = qt * QT + lax.broadcasted_iota(jnp.int32, (1, 2 * QT), 1) % QT
        qstart = doc_start(bounds, qpos)
        s = dot(k, q2, NT) * c2 - l2
        s = jnp.where((kpos <= qpos) & (kpos >= qstart), s, NEG_BIG)
        p = jnp.exp2(s).astype(BF16)
        dp = dot(v, do2, NT)
        ds = (p.astype(F32) * (dp - delta)).astype(BF16)
        dv_ref[...] += dot(p, do2, NN)
        dk_ref[...] += dot(ds, q2, NN)

    dkv_ref[:, :hd] = (dk_ref[...] * scale).astype(BF16)
    dkv_ref[:, hd:] = dv_ref[...].astype(BF16)


def attn_kv(sc, kv, ld_all, qd_all, n_dev, scale):
    rows, two_hd = kv.shape
    hd = two_hd // 2
    work = 4 * 2 * rows * two_hd * rows * n_dev // 2
    return pl.pallas_call(
        functools.partial(attn_kv_kernel, n_dev, scale),
        grid_spec=pltpu.PrefetchScalarGridSpec(
            num_scalar_prefetch=1,
            grid=(2,),
            in_specs=[
                pl.BlockSpec((PIECE, two_hd), lambda g, sc: (g, 0)),
                pl.BlockSpec(ld_all.shape, lambda g, sc: (0, 0, 0)),
                pl.BlockSpec(memory_space=pl.ANY),
            ],
            out_specs=pl.BlockSpec((PIECE, two_hd), lambda g, sc: (g, 0)),
            scratch_shapes=[
                pltpu.VMEM((2 * n_dev, PIECE, qd_all.shape[1]), BF16),
                pltpu.VMEM((PIECE, hd), F32),
                pltpu.VMEM((PIECE, hd), F32),
                pltpu.SemaphoreType.DMA,
            ],
        ),
        out_shape=jax.ShapeDtypeStruct((rows, two_hd), BF16),
        compiler_params=pltpu.CompilerParams(vmem_limit_bytes=VMEM_LIMIT, dimension_semantics=("arbitrary",)),
        cost_estimate=pl.CostEstimate(flops=work, bytes_accessed=16 * rows * two_hd, transcendentals=0),
        name="attn_kv",
    )(sc, kv, ld_all, qd_all)


def solution(mesh):
    n_dev = mesh.shape['cp']
    row_spec = P(('dp', 'cp'))
    full_spec = P()

    def local_layer(x_in, dy_in, doc_id, w_q, w_k, w_v, w_o):
        d_model = x_in.shape[1]
        hd = w_q.shape[2]
        scale = hd ** -0.5
        wk = w_k.reshape(d_model, hd)
        wv = w_v.reshape(d_model, hd)
        wq = w_q.reshape(d_model, 2 * hd)
        wo = w_o.reshape(2 * hd, d_model)
        kv = kv_proj(x_in, wk, wv)
        kv_all = lax.all_gather(kv, 'cp', axis=0, tiled=True)
        counts = jnp.sum((doc_id[None, :] < jnp.arange(1, 5, dtype=jnp.int32)[:, None]).astype(jnp.int32), axis=1)
        bounds = lax.psum(counts, 'cp')
        me = lax.axis_index('cp').astype(jnp.int32)
        sc = jnp.concatenate([me[None], bounds])
        q = dot(x_in, wq, NN).astype(BF16)
        do = dot(dy_in, wo, NT).astype(BF16)
        qd_all = lax.all_gather(jnp.concatenate([q, do], axis=1), 'cp', axis=0, tiled=True)
        o, dq, ld = attn_q(sc, q, do, kv_all, n_dev, scale)
        ld_all = lax.all_gather(ld, 'cp', axis=0, tiled=True)
        y_out = dot(o, wo, NN).astype(BF16)
        dkv = attn_kv(sc, kv, ld_all, qd_all, n_dev, scale)
        dx = dot(dq, wq, NT) + dot(dkv[:, :hd], wk, NT) + dot(dkv[:, hd:], wv, NT)
        return y_out, dx.astype(BF16)

    return jax.shard_map(local_layer, mesh=mesh,
                         in_specs=(row_spec, row_spec, row_spec, full_spec, full_spec, full_spec, full_spec),
                         out_specs=(row_spec, row_spec), check_vma=False)
```

```python
import functools
import math

import jax
import jax.numpy as jnp
from jax import lax
from jax.experimental import pallas as pl
from jax.experimental.pallas import tpu as pltpu
from jax.sharding import PartitionSpec as P

NEG_BIG = -1.0e30
BF16 = jnp.bfloat16
F32 = jnp.float32
PIECE = 512
QT = 256
NT = (((1,), (1,)), ((), ()))
NN = (((1,), (0,)), ((), ()))
VMEM_LIMIT = 60 * 1024 * 1024
MESH = pl.DeviceIdType.MESH
ANY = pl.BlockSpec(memory_space=pl.ANY)
VMEM = pl.BlockSpec(memory_space=pltpu.VMEM)


def dot(a, b, dims):
    return lax.dot_general(a, b, dims, preferred_element_type=F32)


def doc_start(bounds, pos):
    out = jnp.zeros_like(pos)
    for b in bounds:
        out = jnp.maximum(out, jnp.where(b <= pos, b, 0))
    return out


def doc_end(bounds, pos, seq_len):
    out = seq_len
    for b in bounds:
        out = jnp.minimum(out, jnp.where(b > pos, b, seq_len))
    return out


def neighbours(me):
    return me + 2 - 4 * ((me // 2) % 2), me + 4 - 8 * (me // 4), me + 1 - 2 * (me % 2)


def entry_barrier(me, n_dev):
    barrier = pltpu.get_barrier_semaphore()
    for d in range(1, n_dev):
        pl.semaphore_signal(barrier, inc=1, device_id={'cp': lax.rem(me + d, n_dev)}, device_id_type=MESH)
    pl.semaphore_wait(barrier, n_dev - 1)


def broadcast_copies(me, n_dev, src, dst, send_sem, recv_sem):
    return [
        pltpu.make_async_remote_copy(
            src_ref=src, dst_ref=dst.at[me], send_sem=send_sem.at[d - 1], recv_sem=recv_sem.at[d - 1],
            device_id={'cp': lax.rem(me + d, n_dev)}, device_id_type=MESH)
        for d in range(1, n_dev)
    ]


def proj_gather_kernel(n_dev, x_hbm, dy_hbm, doc_ref, wq_hbm, wk_hbm, wv_hbm, wo_hbm,
                       kvg, qe_hbm, ql_hbm, pe_hbm, pl_hbm, docg_ref,
                       x_s, dy_s, wq_s, wk_s, wv_s, wo_s, kv_s, qd_s,
                       w_sem, x_sem, dy_sem, send_sem, recv_sem, qsend_sem, qrecv_sem, loc_sem, dsend_sem, drecv_sem):
    me = lax.axis_index('cp')
    px, py, pc = neighbours(me)
    pd = px + py - me
    last = 2 * n_dev - 1
    hd = wk_s.shape[1]
    tiles = PIECE // QT

    w_copies = [pltpu.make_async_copy(a, b, w_sem.at[n]) for n, (a, b) in enumerate(
        ((wk_hbm, wk_s), (wv_hbm, wv_s), (wq_hbm, wq_s), (wo_hbm, wo_s)))]

    def row_copy(src, dst, sem, tile):
        rows = pl.ds(pl.multiple_of(tile * QT, QT), QT)
        return pltpu.make_async_copy(src.at[rows], dst.at[rows], sem.at[tile])

    w_copies[0].start()
    row_copy(x_hbm, x_s, x_sem, 0).start()
    w_copies[1].start()
    for t in range(1, 2 * tiles):
        row_copy(x_hbm, x_s, x_sem, t).start()
    w_copies[2].start()
    w_copies[3].start()
    for t in range(2 * tiles):
        row_copy(dy_hbm, dy_s, dy_sem, t).start()

    entry_barrier(me, n_dev)
    docg_ref[me] = doc_ref[...]
    doc_copies = broadcast_copies(me, n_dev, doc_ref, docg_ref, dsend_sem, drecv_sem)
    for cp in doc_copies:
        cp.start()

    def send(n, src, piece, peer):
        return pltpu.make_async_remote_copy(
            src_ref=src, dst_ref=kvg.at[piece], send_sem=send_sem.at[n], recv_sem=recv_sem.at[n],
            device_id={'cp': peer}, device_id_type=MESH)

    copies = [
        send(0, kv_s.at[0], me, px), send(1, kv_s.at[1], last - me, px),
        send(2, kv_s.at[0], me, py), send(3, kv_s.at[1], last - me, py),
        send(4, kv_s.at[0], me, pc), send(5, kv_s.at[1], last - me, pc),
        send(6, kvg.at[px], px, py), send(7, kvg.at[last - py], last - py, px),
        send(8, kvg.at[px], px, pc), send(9, kvg.at[last - px], last - px, pc),
        send(10, kvg.at[py], py, pc), send(11, kvg.at[last - py], last - py, pc),
        send(12, kvg.at[pd], pd, pc), send(13, kvg.at[last - pd], last - pd, pc),
    ]
    local = [
        pltpu.make_async_copy(kv_s.at[0], kvg.at[me], loc_sem.at[0]),
        pltpu.make_async_copy(kv_s.at[1], kvg.at[last - me], loc_sem.at[1]),
        pltpu.make_async_copy(qd_s.at[0], qe_hbm, loc_sem.at[2]),
        pltpu.make_async_copy(qd_s.at[1], ql_hbm, loc_sem.at[3]),
    ]
    q_copies = [
        pltpu.make_async_remote_copy(
            src_ref=qd_s.at[n], dst_ref=dst, send_sem=qsend_sem.at[n], recv_sem=qrecv_sem.at[n],
            device_id={'cp': pc}, device_id_type=MESH)
        for n, dst in enumerate((pe_hbm, pl_hbm))
    ]

    def kv_piece(p):
        @pl.loop(0, tiles)
        def _(h):
            row_copy(x_hbm, x_s, x_sem, p * tiles + h).wait()
            rows = pl.ds(pl.multiple_of(p * PIECE + h * QT, QT), QT)
            out = pl.ds(pl.multiple_of(h * QT, QT), QT)
            x = x_s[rows, :]
            kv_s[p, out, 0:hd] = dot(x, wk_s[...], NN).astype(BF16)
            kv_s[p, out, hd:2 * hd] = dot(x, wv_s[...], NN).astype(BF16)

    def qd_piece(p):
        @pl.loop(0, tiles)
        def _(h):
            rows = pl.ds(pl.multiple_of(p * PIECE + h * QT, QT), QT)
            out = pl.ds(pl.multiple_of(h * QT, QT), QT)
            qd_s[p, out, 0:2 * hd] = dot(x_s[rows, :], wq_s[...], NN).astype(BF16)
            row_copy(dy_hbm, dy_s, dy_sem, p * tiles + h).wait()
            qd_s[p, out, 2 * hd:4 * hd] = dot(dy_s[rows, :], wo_s[...], NT).astype(BF16)

    w_copies[0].wait()
    w_copies[1].wait()
    kv_piece(0)
    copies[0].start()
    copies[4].start()
    local[0].start()
    kv_piece(1)
    copies[3].start()
    copies[1].start()
    copies[2].start()
    copies[5].start()
    local[1].start()
    w_copies[2].wait()
    w_copies[3].wait()
    qd_piece(0)
    q_copies[0].start()
    local[2].start()
    qd_piece(1)
    q_copies[1].start()
    local[3].start()
    for arrived, forwards in ((0, (6, 8)), (3, (7, 11)), (1, (9,)), (2, (10,)), (6, (12,)), (7, (13,))):
        copies[arrived].wait_recv()
        for n in forwards:
            copies[n].start()
    for n in (4, 5, 8, 9, 10, 11, 12, 13):
        copies[n].wait_recv()
    for cp in copies:
        cp.wait_send()
    for cp in local:
        cp.wait()
    for cp in q_copies:
        cp.wait()
    for cp in doc_copies:
        cp.wait()


def proj_gather(x, dy, doc, wq, wk, wv, wo, n_dev):
    rows, d = x.shape
    hd = wk.shape[1]
    qd_shape = jax.ShapeDtypeStruct((PIECE, 4 * hd), BF16)
    dma = pltpu.SemaphoreType.DMA
    return pl.pallas_call(
        functools.partial(proj_gather_kernel, n_dev),
        in_specs=[ANY, ANY, VMEM, ANY, ANY, ANY, ANY],
        out_specs=[ANY, ANY, ANY, ANY, ANY, VMEM],
        out_shape=[
            jax.ShapeDtypeStruct((2 * n_dev, PIECE, 2 * hd), BF16),
            qd_shape, qd_shape, qd_shape, qd_shape,
            jax.ShapeDtypeStruct((n_dev,) + doc.shape, jnp.int32),
        ],
        scratch_shapes=[
            pltpu.VMEM((rows, d), BF16), pltpu.VMEM((rows, d), BF16),
            pltpu.VMEM((d, 2 * hd), BF16), pltpu.VMEM((d, hd), BF16), pltpu.VMEM((d, hd), BF16), pltpu.VMEM((2 * hd, d), BF16),
            pltpu.VMEM((2, PIECE, 2 * hd), BF16), pltpu.VMEM((2, PIECE, 4 * hd), BF16),
            dma((4,)), dma((rows // QT,)), dma((rows // QT,)), dma((14,)), dma((14,)), dma((2,)), dma((2,)), dma((4,)),
            dma((n_dev - 1,)), dma((n_dev - 1,)),
        ],
        compiler_params=pltpu.CompilerParams(vmem_limit_bytes=VMEM_LIMIT, collective_id=0, has_side_effects=True),
        cost_estimate=pl.CostEstimate(flops=12 * rows * d * hd, bytes_accessed=8 * rows * d, transcendentals=0),
        name="proj_gather",
    )(x, dy, doc, wq, wk, wv, wo)


def ld_gather_kernel(n_dev, ld_ref, out_ref, send_sem, recv_sem):
    me = lax.axis_index('cp')
    entry_barrier(me, n_dev)
    out_ref[me] = ld_ref[...]
    copies = broadcast_copies(me, n_dev, ld_ref, out_ref, send_sem, recv_sem)
    for cp in copies:
        cp.start()
    for cp in copies:
        cp.wait()


def ld_gather(ld, n_dev):
    return pl.pallas_call(
        functools.partial(ld_gather_kernel, n_dev),
        in_specs=[VMEM], out_specs=VMEM,
        out_shape=jax.ShapeDtypeStruct((n_dev,) + ld.shape, F32),
        scratch_shapes=[pltpu.SemaphoreType.DMA((n_dev - 1,)), pltpu.SemaphoreType.DMA((n_dev - 1,))],
        compiler_params=pltpu.CompilerParams(collective_id=1, has_side_effects=True),
        cost_estimate=pl.CostEstimate(flops=10_000_000, bytes_accessed=1 << 20, transcendentals=0),
        name="ld_gather",
    )(ld)


def q_range(sc_ref, n_dev, bounds, t):
    me = sc_ref[0]
    piece = jnp.where(t < 2, me, 2 * n_dev - 1 - me)
    q0 = piece * PIECE + (t % 2) * QT
    return q0, doc_start(bounds, q0) // PIECE, piece + 1


def load_kv(sc_ref, n_dev, bounds, kv_hbm, kv_s, sem):
    me = sc_ref[0]
    late = 2 * n_dev - 1 - me
    lo_e = doc_start(bounds, me * PIECE) // PIECE
    lo_l = doc_start(bounds, late * PIECE) // PIECE
    for act in ("start", "wait"):
        for p in range(2 * n_dev):
            @pl.when(((p >= lo_e) & (p <= me)) | ((p >= lo_l) & (p <= late)))
            def _():
                getattr(pltpu.make_async_copy(kv_hbm.at[p], kv_s.at[p], sem), act)()


def fold_lanes(op, acc, s):
    for j in range(s.shape[1] // 128):
        acc = op(acc, s[:, j * 128:(j + 1) * 128])
    return acc


def stack_heads(ref, lo, hd):
    return jnp.concatenate([ref[:, lo:lo + hd], ref[:, lo + hd:lo + 2 * hd]], axis=0)


def attn_fwd_kernel(n_dev, scale, sc_ref, qe_ref, ql_ref, kv_hbm, o_ref, ld_ref, lcol_ref, dcol_ref, kv_s, s_ref, mx_ref, l_ref, acc_ref, sem):
    t = pl.program_id(0)
    bounds = [sc_ref[1 + d] for d in range(4)]
    hd = acc_ref.shape[1]
    c2 = scale * math.log2(math.e)

    @pl.when(t == 0)
    def _():
        load_kv(sc_ref, n_dev, bounds, kv_hbm, kv_s, sem)

    q0, kt0, kt1 = q_range(sc_ref, n_dev, bounds, t)
    early = t < 2
    q2 = jnp.where(early, stack_heads(qe_ref, 0, hd), stack_heads(ql_ref, 0, hd))
    do2 = jnp.where(early, stack_heads(qe_ref, 2 * hd, hd), stack_heads(ql_ref, 2 * hd, hd))
    rpos = q0 + lax.broadcasted_iota(jnp.int32, (2 * QT, 1), 0) % QT
    rstart = doc_start(bounds, rpos)
    mx_ref[...] = jnp.full(mx_ref.shape, NEG_BIG, F32)

    @pl.loop(kt0, kt1)
    def _(kt):
        s = dot(q2, kv_s[kt, :, :hd], NT) * c2
        kpos = kt * PIECE + lax.broadcasted_iota(jnp.int32, (1, PIECE), 1)
        s = jnp.where((kpos <= rpos) & (kpos >= rstart), s, NEG_BIG)
        s_ref[kt] = s
        mx_ref[...] = fold_lanes(jnp.maximum, mx_ref[...], s)

    m = jnp.max(mx_ref[...], axis=1, keepdims=True)
    l_ref[...] = jnp.zeros(l_ref.shape, F32)
    acc_ref[...] = jnp.zeros(acc_ref.shape, F32)

    @pl.loop(kt0, kt1)
    def _(kt):
        p = jnp.exp2(s_ref[kt] - m)
        l_ref[...] = fold_lanes(jnp.add, l_ref[...], p)
        acc_ref[...] += dot(p.astype(BF16), kv_s[kt, :, hd:], NN)

    l = jnp.sum(l_ref[...], axis=1, keepdims=True)
    o2 = (acc_ref[...] * (1.0 / l)).astype(BF16)
    o_ref[:, :hd] = o2[:QT]
    o_ref[:, hd:] = o2[QT:]
    delta = jnp.sum(do2.astype(F32) * o2.astype(F32), axis=1, keepdims=True)
    l2 = jnp.broadcast_to(m + jnp.log2(l), (2 * QT, 128))
    delta = jnp.broadcast_to(delta, (2 * QT, 128))
    lcol_ref[0] = l2
    dcol_ref[0] = delta
    ld_ref[0, 0:1] = jnp.transpose(l2)[0:1]
    ld_ref[0, 1:2] = jnp.transpose(delta)[0:1]


def attn_fwd(sc, qe, ql, kvg, n_dev, scale):
    hd = kvg.shape[2] // 2
    rows = 2 * PIECE
    nt = rows // QT
    col = pl.BlockSpec((1, 2 * QT, 128), lambda t, sc: (t, 0, 0))
    col_shape = jax.ShapeDtypeStruct((nt, 2 * QT, 128), F32)
    return pl.pallas_call(
        functools.partial(attn_fwd_kernel, n_dev, scale),
        grid_spec=pltpu.PrefetchScalarGridSpec(
            num_scalar_prefetch=1,
            grid=(nt,),
            in_specs=[
                pl.BlockSpec((QT, 4 * hd), lambda t, sc: (jnp.minimum(t, 1), 0)),
                pl.BlockSpec((QT, 4 * hd), lambda t, sc: (jnp.maximum(t - 2, 0), 0)),
                ANY,
            ],
            out_specs=[
                pl.BlockSpec((QT, 2 * hd), lambda t, sc: (t, 0)),
                pl.BlockSpec((1, 2, 2 * QT), lambda t, sc: (t, 0, 0)),
                col, col,
            ],
            scratch_shapes=[
                pltpu.VMEM(kvg.shape, BF16),
                pltpu.VMEM((2 * n_dev, 2 * QT, PIECE), F32),
                pltpu.VMEM((2 * QT, 128), F32),
                pltpu.VMEM((2 * QT, 128), F32),
                pltpu.VMEM((2 * QT, hd), F32),
                pltpu.SemaphoreType.DMA,
            ],
        ),
        out_shape=[
            jax.ShapeDtypeStruct((rows, 2 * hd), BF16),
            jax.ShapeDtypeStruct((nt, 2, 2 * QT), F32),
            col_shape, col_shape,
        ],
        compiler_params=pltpu.CompilerParams(vmem_limit_bytes=VMEM_LIMIT, dimension_semantics=("arbitrary",)),
        cost_estimate=pl.CostEstimate(flops=16 * rows * rows * hd * n_dev // 4, bytes_accessed=1 << 23, transcendentals=0),
        name="attn_fwd",
    )(sc, qe, ql, kvg)


def attn_dq_kernel(n_dev, scale, sc_ref, qe_ref, ql_ref, lcol_ref, dcol_ref, kv_hbm, dq_ref, kv_s, acc_ref, sem):
    t = pl.program_id(0)
    bounds = [sc_ref[1 + d] for d in range(4)]
    hd = acc_ref.shape[1]
    c2 = scale * math.log2(math.e)

    @pl.when(t == 0)
    def _():
        load_kv(sc_ref, n_dev, bounds, kv_hbm, kv_s, sem)

    q0, kt0, kt1 = q_range(sc_ref, n_dev, bounds, t)
    early = t < 2
    q2 = jnp.where(early, stack_heads(qe_ref, 0, hd), stack_heads(ql_ref, 0, hd))
    do2 = jnp.where(early, stack_heads(qe_ref, 2 * hd, hd), stack_heads(ql_ref, 2 * hd, hd))
    rpos = q0 + lax.broadcasted_iota(jnp.int32, (2 * QT, 1), 0) % QT
    rstart = doc_start(bounds, rpos)
    l2 = lcol_ref[0, :, 0:1]
    delta = dcol_ref[0, :, 0:1]
    acc_ref[...] = jnp.zeros(acc_ref.shape, F32)

    @pl.loop(kt0, kt1)
    def _(kt):
        k = kv_s[kt, :, :hd]
        s = dot(q2, k, NT) * c2 - l2
        kpos = kt * PIECE + lax.broadcasted_iota(jnp.int32, (1, PIECE), 1)
        s = jnp.where((kpos <= rpos) & (kpos >= rstart), s, NEG_BIG)
        p = jnp.exp2(s).astype(BF16).astype(F32)
        dp = dot(do2, kv_s[kt, :, hd:], NT)
        ds = (p * (dp - delta)).astype(BF16)
        acc_ref[...] += dot(ds, k, NN)

    dq2 = (acc_ref[...] * scale).astype(BF16)
    dq_ref[:, :hd] = dq2[:QT]
    dq_ref[:, hd:] = dq2[QT:]


def attn_dq(sc, qe, ql, lcol, dcol, kvg, n_dev, scale):
    hd = kvg.shape[2] // 2
    rows = 2 * PIECE
    nt = rows // QT
    col = pl.BlockSpec((1, 2 * QT, 128), lambda t, sc: (t, 0, 0))
    return pl.pallas_call(
        functools.partial(attn_dq_kernel, n_dev, scale),
        grid_spec=pltpu.PrefetchScalarGridSpec(
            num_scalar_prefetch=1,
            grid=(nt,),
            in_specs=[
                pl.BlockSpec((QT, 4 * hd), lambda t, sc: (jnp.minimum(t, 1), 0)),
                pl.BlockSpec((QT, 4 * hd), lambda t, sc: (jnp.maximum(t - 2, 0), 0)),
                col, col, ANY,
            ],
            out_specs=pl.BlockSpec((QT, 2 * hd), lambda t, sc: (t, 0)),
            scratch_shapes=[
                pltpu.VMEM(kvg.shape, BF16),
                pltpu.VMEM((2 * QT, hd), F32),
                pltpu.SemaphoreType.DMA,
            ],
        ),
        out_shape=jax.ShapeDtypeStruct((rows, 2 * hd), BF16),
        compiler_params=pltpu.CompilerParams(vmem_limit_bytes=VMEM_LIMIT, dimension_semantics=("arbitrary",)),
        cost_estimate=pl.CostEstimate(flops=24 * rows * rows * hd * n_dev // 4, bytes_accessed=1 << 23, transcendentals=0),
        name="attn_dq",
    )(sc, qe, ql, lcol, dcol, kvg)


def attn_kv_kernel(n_dev, scale, own, sc_ref, ld_ref, kv_ref, *refs):
    n_in = 10 if own else 4
    qd_in, (out_ref, qd_s, dk_ref, dv_ref, sem) = refs[:n_in], refs[n_in:]
    g = pl.program_id(0)
    me = sc_ref[0]
    bounds = [sc_ref[1 + d] for d in range(4)]
    hd = dk_ref.shape[1]
    seq_len = 2 * n_dev * PIECE
    last = 2 * n_dev - 1
    c2 = scale * math.log2(math.e)
    chip, core = me // 2, me % 2
    x_chip = chip + 1 - 2 * (chip % 2)
    y_chip = chip + 2 - 4 * (chip // 2)
    d_chip = x_chip + y_chip - chip
    par = me + 1 - 2 * core

    pieces = [(me, True), (last - me, True), (par, True), (last - par, True)]
    if own:
        for c in (x_chip, y_chip, d_chip):
            for same in (True, False):
                dev = 2 * c + (core if same else 1 - core)
                pieces.append((last - dev, c < chip))
        first_key = me * PIECE
    else:
        first_key = core * PIECE
    reach = doc_end(bounds, (last - me) * PIECE + PIECE - 1, seq_len) if own else seq_len
    reach_e = doc_end(bounds, me * PIECE + PIECE - 1, seq_len) if own else seq_len

    def wanted(piece):
        if own:
            return ((piece >= me) & (piece * PIECE < reach_e)) | ((piece >= last - me) & (piece * PIECE < reach))
        return piece >= 2 * chip

    @pl.when(g == 0)
    def _():
        for act in ("start", "wait"):
            for ref, (piece, valid) in zip(qd_in, pieces):
                @pl.when(valid & wanted(piece))
                def _():
                    getattr(pltpu.make_async_copy(ref, qd_s.at[piece], sem), act)()

    if own:
        kp = jnp.where(g == 0, me, last - me)
        a0 = jnp.where(g == 0, 2 * me, 4 * chip + 4)
        b0 = jnp.where(g == 0, 2 * (last - 1 - 2 * chip), 2 * (last - me))
        b1 = 2 * (last + 1)
        live = True
    else:
        tgt = jnp.where(g == 0, x_chip, jnp.where(g == 1, y_chip, d_chip))
        kp = 2 * tgt + core
        a0 = 4 * chip
        b0 = 2 * (last - 1 - 2 * chip)
        b1 = 2 * (last + 1 - 2 * chip)
        live = tgt < chip
    a1 = 4 * chip + 4
    end = (doc_end(bounds, kp * PIECE + PIECE - 1, seq_len) + QT - 1) // QT
    k = kv_ref[0, :, :hd]
    v = kv_ref[0, :, hd:]
    kpos = kp * PIECE + lax.broadcasted_iota(jnp.int32, (PIECE, 1), 0)
    dk_ref[...] = jnp.zeros(dk_ref.shape, F32)
    dv_ref[...] = jnp.zeros(dv_ref.shape, F32)
    na = jnp.maximum(jnp.minimum(a1, end) - a0, 0)
    nb = jnp.maximum(jnp.minimum(b1, end) - b0, 0)

    @pl.loop(0, jnp.where(live, na + nb, 0))
    def _(i):
        qt = jnp.where(i < na, a0 + i, b0 + i - na)
        qp = qt // 2
        half = qt % 2
        late = qp >= n_dev
        tile = jnp.where(late, (last - qp) * 4 + 2, qp * 4) + half
        rows = pl.ds(pl.multiple_of(half * QT, QT), QT)
        q2 = jnp.concatenate([qd_s[qp, rows, 0:hd], qd_s[qp, rows, hd:2 * hd]], axis=0)
        do2 = jnp.concatenate([qd_s[qp, rows, 2 * hd:3 * hd], qd_s[qp, rows, 3 * hd:4 * hd]], axis=0)
        l2 = ld_ref[tile, 0:1, :]
        delta = ld_ref[tile, 1:2, :]
        qpos = qt * QT + lax.broadcasted_iota(jnp.int32, (1, 2 * QT), 1) % QT
        qstart = doc_start(bounds, qpos)
        s = dot(k, q2, NT) * c2 - l2
        s = jnp.where((kpos <= qpos) & (kpos >= qstart), s, NEG_BIG)
        p = jnp.exp2(s).astype(BF16)
        dp = dot(v, do2, NT)
        ds = (p.astype(F32) * (dp - delta)).astype(BF16)
        dv_ref[...] += dot(p, do2, NN)
        dk_ref[...] += dot(ds, q2, NN)

    out_ref[0, :, :hd] = dk_ref[...] * scale
    out_ref[0, :, hd:] = dv_ref[...]


def attn_kv(own, sc, ld_all, kvg, qds, n_dev, scale):
    two_hd = kvg.shape[2]
    hd = two_hd // 2
    n_key = 2 if own else 3
    last = 2 * n_dev - 1

    def kv_block(g, sc):
        me = sc[0]
        if own:
            return (jnp.where(g == 0, me, last - me), 0, 0)
        chip, core = me // 2, me % 2
        x_chip = chip + 1 - 2 * (chip % 2)
        y_chip = chip + 2 - 4 * (chip // 2)
        tgt = jnp.where(g == 0, x_chip, jnp.where(g == 1, y_chip, x_chip + y_chip - chip))
        return (2 * tgt + core, 0, 0)

    return pl.pallas_call(
        functools.partial(attn_kv_kernel, n_dev, scale, own),
        grid_spec=pltpu.PrefetchScalarGridSpec(
            num_scalar_prefetch=1,
            grid=(n_key,),
            in_specs=[
                pl.BlockSpec(ld_all.shape, lambda g, sc: (0, 0, 0)),
                pl.BlockSpec((1, PIECE, two_hd), kv_block),
            ] + [ANY] * len(qds),
            out_specs=pl.BlockSpec((1, PIECE, two_hd), lambda g, sc: (g, 0, 0)),
            scratch_shapes=[
                pltpu.VMEM((2 * n_dev, PIECE, 4 * hd), BF16),
                pltpu.VMEM((PIECE, hd), F32),
                pltpu.VMEM((PIECE, hd), F32),
                pltpu.SemaphoreType.DMA,
            ],
        ),
        out_shape=jax.ShapeDtypeStruct((n_key, PIECE, two_hd), F32),
        compiler_params=pltpu.CompilerParams(vmem_limit_bytes=VMEM_LIMIT, dimension_semantics=("arbitrary",)),
        cost_estimate=pl.CostEstimate(flops=(24 if own else 8) * PIECE * PIECE * hd * 16, bytes_accessed=1 << 23, transcendentals=0),
        name="attn_kv_own" if own else "attn_kv_back",
    )(sc, ld_all, kvg, *qds)


def dx_kernel(dq_ref, own_ref, rx_ref, ry_ref, rd_ref, wq_ref, wk_ref, wv_ref, dx_ref, lhs):
    hd = wk_ref.shape[1]

    @pl.when(pl.program_id(0) == 0)
    def _():
        lhs[:, :2 * hd] = dq_ref[...]
        lhs[:PIECE, 2 * hd:] = (own_ref[0] + rx_ref[...] + ry_ref[...] + rd_ref[...]).astype(BF16)
        lhs[PIECE:, 2 * hd:] = own_ref[1].astype(BF16)

    w = jnp.concatenate([wq_ref[...], wk_ref[...], wv_ref[...]], axis=1)
    for r in range(2):
        rows = slice(r * PIECE, (r + 1) * PIECE)
        dx_ref[rows, :] = dot(lhs[rows, :], w, NT).astype(BF16)


def dx_proj(dq, own, rx, ry, rd, wq, wk, wv):
    rows, qd = dq.shape
    d, hd = wk.shape
    nb = d // 512
    full = lambda a: pl.BlockSpec(a.shape, lambda j: (0,) * a.ndim)
    return pl.pallas_call(
        dx_kernel,
        grid=(nb,),
        in_specs=[full(dq), full(own), full(rx), full(ry), full(rd),
                  pl.BlockSpec((512, qd), lambda j: (j, 0)),
                  pl.BlockSpec((512, hd), lambda j: (j, 0)),
                  pl.BlockSpec((512, hd), lambda j: (j, 0))],
        out_specs=pl.BlockSpec((rows, 512), lambda j: (0, j)),
        out_shape=jax.ShapeDtypeStruct((rows, d), BF16),
        scratch_shapes=[pltpu.VMEM((rows, 2 * qd), BF16)],
        compiler_params=pltpu.CompilerParams(vmem_limit_bytes=VMEM_LIMIT, dimension_semantics=("arbitrary",)),
        cost_estimate=pl.CostEstimate(flops=4 * rows * d * qd, bytes_accessed=4 * rows * d, transcendentals=0),
        name="dx_proj",
    )(dq, own, rx, ry, rd, wq, wk, wv)


def solution(mesh):
    n_dev = mesh.shape['cp']
    row_spec = P(('dp', 'cp'))
    full_spec = P()

    def chip_pairs(pairs):
        return [(2 * a + c, 2 * b + c) for a, b in pairs for c in (0, 1)]

    up_x, up_y, up_d = (chip_pairs(p) for p in ([(0, 1), (2, 3)], [(0, 2), (1, 3)], [(0, 3), (1, 2)]))

    def back(pairs):
        return [(b, a) for a, b in pairs]

    def swap(pairs):
        return [(b, b + 1 - 2 * (b % 2)) for _, b in pairs]

    def local_layer(x_in, dy_in, doc_id, w_q, w_k, w_v, w_o):
        d_model = x_in.shape[1]
        hd = w_q.shape[2]
        scale = hd ** -0.5
        wk = w_k.reshape(d_model, hd)
        wv = w_v.reshape(d_model, hd)
        wq = w_q.reshape(d_model, 2 * hd)
        wo = w_o.reshape(2 * hd, d_model)
        kvg, qe, ql, pe, pl_, docg = proj_gather(x_in, dy_in, doc_id.reshape(8, -1), wq, wk, wv, wo, n_dev)
        bounds = jnp.sum((docg.reshape(1, -1) < jnp.arange(1, 5, dtype=jnp.int32)[:, None]).astype(jnp.int32), axis=1)
        sc = jnp.concatenate([lax.axis_index('cp').astype(jnp.int32)[None], bounds])
        ups = []
        for pairs in (up_x, up_y, up_d):
            a = lax.ppermute(ql, 'cp', pairs)
            ups += [a, lax.ppermute(a, 'cp', swap(pairs))]
        o, ld, lcol, dcol = attn_fwd(sc, qe, ql, kvg, n_dev, scale)
        ld_all = ld_gather(ld, n_dev).reshape(-1, ld.shape[1], ld.shape[2])
        ret = attn_kv(False, sc, ld_all, kvg, (qe, ql, pe, pl_), n_dev, scale)
        rx, ry, rd = (lax.ppermute(ret[n], 'cp', back(pairs)) for n, pairs in enumerate((up_x, up_y, up_d)))
        dq = attn_dq(sc, qe, ql, lcol, dcol, kvg, n_dev, scale)
        y_out = dot(o, wo, NN).astype(BF16)
        dkv = attn_kv(True, sc, ld_all, kvg, (qe, ql, pe, pl_, *ups), n_dev, scale)
        dx = dx_proj(dq, dkv, rx, ry, rd, wq, wk, wv)
        return y_out, dx

    return jax.shard_map(local_layer, mesh=mesh,
                         in_specs=(row_spec, row_spec, row_spec, full_spec, full_spec, full_spec, full_spec),
                         out_specs=(row_spec, row_spec), check_vma=False)
```

```python
import functools
import math

import jax
import jax.numpy as jnp
from jax import lax
from jax.experimental import pallas as pl
from jax.experimental.pallas import tpu as pltpu
from jax.sharding import PartitionSpec as P

NEG_BIG = -1.0e30
BF16 = jnp.bfloat16
F32 = jnp.float32
PIECE = 512
ROWS = 256
LANES = 128
NT = (((1,), (1,)), ((), ()))
NN = (((1,), (0,)), ((), ()))
VMEM_LIMIT = 60 * 1024 * 1024
MESH = pl.DeviceIdType.MESH
ANY = pl.BlockSpec(memory_space=pl.ANY)
VMEM = pl.BlockSpec(memory_space=pltpu.VMEM)


def dot(a, b, dims):
    return lax.dot_general(a, b, dims, preferred_element_type=F32)


def doc_start(bounds, pos):
    out = jnp.zeros_like(pos)
    for b in bounds:
        out = jnp.maximum(out, jnp.where(b <= pos, b, 0))
    return out


def doc_end(bounds, pos, seq_len):
    out = seq_len
    for b in bounds:
        out = jnp.minimum(out, jnp.where(b > pos, b, seq_len))
    return out


def neighbours(me):
    return me + 2 - 4 * ((me // 2) % 2), me + 4 - 8 * (me // 4), me + 1 - 2 * (me % 2)


def entry_barrier(me, n_dev):
    barrier = pltpu.get_barrier_semaphore()
    for d in range(1, n_dev):
        pl.semaphore_signal(barrier, inc=1, device_id={'cp': lax.rem(me + d, n_dev)}, device_id_type=MESH)
    pl.semaphore_wait(barrier, n_dev - 1)


def broadcast_copies(me, n_dev, src, dst, send_sem, recv_sem):
    return [
        pltpu.make_async_remote_copy(
            src_ref=src, dst_ref=dst.at[me], send_sem=send_sem.at[d - 1], recv_sem=recv_sem.at[d - 1],
            device_id={'cp': lax.rem(me + d, n_dev)}, device_id_type=MESH)
        for d in range(1, n_dev)
    ]


def proj_gather_kernel(n_dev, x_hbm, dy_hbm, doc_ref, wq_hbm, wk_hbm, wv_hbm, wo_hbm,
                       kvg, own_hbm, par_hbm, up_hbm, w_hbm, docg_ref,
                       x_s, dy_s, wq_s, w_s, wo_s, kv_s, qd_s,
                       w_sem, x_sem, dy_sem, send_sem, recv_sem, qsend_sem, qrecv_sem, loc_sem, dsend_sem, drecv_sem):
    me = lax.axis_index('cp')
    px, py, pc = neighbours(me)
    pd = px + py - me
    last = 2 * n_dev - 1
    hd = wq_s.shape[2]
    qd = 2 * hd
    tiles = PIECE // ROWS

    w_copies = [pltpu.make_async_copy(a, b, w_sem.at[n]) for n, (a, b) in enumerate(
        ((wk_hbm, w_s.at[:, pl.ds(qd, hd)]), (wv_hbm, w_s.at[:, pl.ds(qd + hd, hd)]), (wq_hbm, wq_s), (wo_hbm, wo_s)))]

    def row_copy(src, dst, sem, tile):
        rows = pl.ds(pl.multiple_of(tile * ROWS, ROWS), ROWS)
        return pltpu.make_async_copy(src.at[rows], dst.at[rows], sem.at[tile])

    w_copies[0].start()
    w_copies[1].start()
    for t in range(2 * tiles):
        row_copy(x_hbm, x_s, x_sem, t).start()
    w_copies[2].start()
    w_copies[3].start()
    for t in range(2 * tiles):
        row_copy(dy_hbm, dy_s, dy_sem, t).start()

    entry_barrier(me, n_dev)
    docg_ref[me] = doc_ref[...]
    doc_copies = broadcast_copies(me, n_dev, doc_ref, docg_ref, dsend_sem, drecv_sem)
    for cp in doc_copies:
        cp.start()

    hops = (
        (kv_s.at[0], me, px), (kv_s.at[1], last - me, px),
        (kv_s.at[0], me, py), (kv_s.at[1], last - me, py),
        (kv_s.at[0], me, pc), (kv_s.at[1], last - me, pc),
        (kvg.at[px], px, py), (kvg.at[last - py], last - py, px),
        (kvg.at[px], px, pc), (kvg.at[last - px], last - px, pc),
        (kvg.at[py], py, pc), (kvg.at[last - py], last - py, pc),
        (kvg.at[pd], pd, pc), (kvg.at[last - pd], last - pd, pc),
    )
    copies = [
        pltpu.make_async_remote_copy(
            src_ref=src, dst_ref=kvg.at[piece], send_sem=send_sem.at[n], recv_sem=recv_sem.at[n],
            device_id={'cp': peer}, device_id_type=MESH)
        for n, (src, piece, peer) in enumerate(hops)
    ]
    local = [pltpu.make_async_copy(src, dst, loc_sem.at[n]) for n, (src, dst) in enumerate((
        (kv_s.at[0], kvg.at[me]), (kv_s.at[1], kvg.at[last - me]), (qd_s.at[0], own_hbm.at[0]), (qd_s.at[1], own_hbm.at[1]), (qd_s.at[1], up_hbm), (w_s, w_hbm)))]
    q_copies = [
        pltpu.make_async_remote_copy(
            src_ref=qd_s.at[n], dst_ref=par_hbm.at[n], send_sem=qsend_sem.at[n], recv_sem=qrecv_sem.at[n],
            device_id={'cp': pc}, device_id_type=MESH)
        for n in range(2)
    ]

    def kv_piece(p):
        @pl.loop(0, tiles)
        def _(h):
            row_copy(x_hbm, x_s, x_sem, p * tiles + h).wait()
            rows = pl.ds(pl.multiple_of(p * PIECE + h * ROWS, ROWS), ROWS)
            out = pl.ds(pl.multiple_of(h * ROWS, ROWS), ROWS)
            kv_s[p, out, :] = dot(x_s[rows, :], w_s[:, qd:], NN).astype(BF16)

    def qd_piece(p):
        @pl.loop(0, tiles)
        def _(h):
            rows = pl.ds(pl.multiple_of(p * PIECE + h * ROWS, ROWS), ROWS)
            out = pl.ds(pl.multiple_of(h * ROWS, ROWS), ROWS)
            qd_s[p, out, 0:qd] = dot(x_s[rows, :], w_s[:, :qd], NN).astype(BF16)
            row_copy(dy_hbm, dy_s, dy_sem, p * tiles + h).wait()
            qd_s[p, out, qd:] = dot(dy_s[rows, :], wo_s[...], NT).astype(BF16)

    w_copies[0].wait()
    w_copies[1].wait()
    kv_piece(0)
    copies[0].start()
    copies[4].start()
    local[0].start()
    kv_piece(1)
    for n in (3, 1, 2, 5):
        copies[n].start()
    local[1].start()
    w_copies[2].wait()

    @pl.loop(0, wq_s.shape[0] // PIECE)
    def _(n):
        rows = pl.ds(pl.multiple_of(n * PIECE, PIECE), PIECE)
        w_s[rows, 0:hd] = wq_s[rows, 0, :]
        w_s[rows, hd:qd] = wq_s[rows, 1, :]

    w_copies[3].wait()
    qd_piece(0)
    q_copies[0].start()
    local[2].start()
    qd_piece(1)
    q_copies[1].start()
    for n in (3, 4, 5):
        local[n].start()
    for arrived, forwards in ((0, (6, 8)), (3, (7, 11)), (1, (9,)), (2, (10,)), (6, (12,)), (7, (13,))):
        copies[arrived].wait_recv()
        for n in forwards:
            copies[n].start()
    for n in (4, 5, 8, 9, 10, 11, 12, 13):
        copies[n].wait_recv()
    for cp in copies:
        cp.wait_send()
    for cp in local + q_copies + doc_copies:
        cp.wait()


def proj_gather(x, dy, doc, wq, wk, wv, wo, n_dev):
    rows, d = x.shape
    hd = wk.shape[1]
    qd_shape = jax.ShapeDtypeStruct((2, PIECE, 4 * hd), BF16)
    dma = pltpu.SemaphoreType.DMA
    n_tile = rows // ROWS
    return pl.pallas_call(
        functools.partial(proj_gather_kernel, n_dev),
        in_specs=[ANY, ANY, VMEM, ANY, ANY, ANY, ANY],
        out_specs=[ANY] * 5 + [VMEM],
        out_shape=[
            jax.ShapeDtypeStruct((2 * n_dev, PIECE, 2 * hd), BF16),
            qd_shape, qd_shape, jax.ShapeDtypeStruct((PIECE, 4 * hd), BF16),
            jax.ShapeDtypeStruct((d, 4 * hd), BF16),
            jax.ShapeDtypeStruct((n_dev,) + doc.shape, jnp.int32),
        ],
        scratch_shapes=[
            pltpu.VMEM((rows, d), BF16), pltpu.VMEM((rows, d), BF16),
            pltpu.VMEM(wq.shape, BF16), pltpu.VMEM((d, 4 * hd), BF16), pltpu.VMEM((2 * hd, d), BF16),
            pltpu.VMEM((2, PIECE, 2 * hd), BF16), pltpu.VMEM((2, PIECE, 4 * hd), BF16),
            *(dma((n,)) for n in (4, n_tile, n_tile, 14, 14, 2, 2, 6, n_dev - 1, n_dev - 1)),
        ],
        compiler_params=pltpu.CompilerParams(vmem_limit_bytes=VMEM_LIMIT, collective_id=0, has_side_effects=True),
        cost_estimate=pl.CostEstimate(flops=12 * rows * d * hd, bytes_accessed=8 * rows * d, transcendentals=0),
        name="proj_gather",
    )(x, dy, doc, wq, wk, wv, wo)


def ld_gather_kernel(n_dev, ld_ref, out_ref, send_sem, recv_sem):
    me = lax.axis_index('cp')
    entry_barrier(me, n_dev)
    out_ref[me] = ld_ref[...]
    copies = broadcast_copies(me, n_dev, ld_ref, out_ref, send_sem, recv_sem)
    for cp in copies:
        cp.start()
    for cp in copies:
        cp.wait()


def ld_gather(ld, n_dev):
    return pl.pallas_call(
        functools.partial(ld_gather_kernel, n_dev),
        in_specs=[VMEM], out_specs=VMEM,
        out_shape=jax.ShapeDtypeStruct((n_dev,) + ld.shape, F32),
        scratch_shapes=[pltpu.SemaphoreType.DMA((n_dev - 1,)), pltpu.SemaphoreType.DMA((n_dev - 1,))],
        compiler_params=pltpu.CompilerParams(collective_id=1, has_side_effects=True),
        cost_estimate=pl.CostEstimate(flops=10_000_000, bytes_accessed=1 << 20, transcendentals=0),
        name="ld_gather",
    )(ld)


class Loader:
    def __init__(self, dst, sem, flag):
        self.dst, self.sem, self.flag = dst, sem, flag

    def copy(self, src, piece):
        return pltpu.make_async_copy(src, self.dst.at[piece], self.sem.at[piece])

    def start(self, src, piece, want):
        self.flag[piece] = jnp.where(want, 1, 0)

        @pl.when(self.flag[piece] == 1)
        def _():
            self.copy(src, piece).start()

    def need(self, src, piece):
        @pl.when(self.flag[piece] == 1)
        def _():
            self.copy(src, piece).wait()
            self.flag[piece] = 0


def loader_scratch(n_piece, width):
    return [pltpu.VMEM((n_piece, PIECE, width), BF16), pltpu.SemaphoreType.DMA((n_piece,)), pltpu.SMEM((n_piece,), jnp.int32)]


def key_range(bounds, piece):
    return doc_start(bounds, piece * PIECE) // PIECE, piece + 1


def start_kv(sc_ref, n_dev, bounds, kv_hbm, kv):
    me = sc_ref[0]
    late = 2 * n_dev - 1 - me
    lo_e, lo_l = key_range(bounds, me)[0], key_range(bounds, late)[0]
    for p in range(2 * n_dev):
        kv.start(kv_hbm.at[p], p, ((p >= lo_e) & (p <= me)) | ((p >= lo_l) & (p <= late)))


def fold_lanes(op, acc, s):
    for j in range(s.shape[1] // LANES):
        acc = op(acc, s[:, j * LANES:(j + 1) * LANES])
    return acc


def stack_heads(a, lo, hd):
    return jnp.concatenate([a[:, lo:lo + hd], a[:, lo + hd:lo + 2 * hd]], axis=0)


def row_pos(first, axis):
    shape = (2 * PIECE, 1) if axis == 0 else (1, 2 * PIECE)
    return first + lax.broadcasted_iota(jnp.int32, shape, axis) % PIECE


def key_pos(first, axis):
    shape = (PIECE, 1) if axis == 0 else (1, PIECE)
    return first + lax.broadcasted_iota(jnp.int32, shape, axis)


def masked_or_not(bounds, q_piece, k_piece, body):
    whole = (k_piece < q_piece) & (doc_start(bounds, q_piece * PIECE + PIECE - 1) <= k_piece * PIECE)

    @pl.when(whole)
    def _():
        body(False)

    @pl.when(jnp.logical_not(whole))
    def _():
        body(True)


def attn_fwd_kernel(n_dev, scale, sc_ref, q_ref, kv_hbm, o_ref, ld_ref, lcol_ref, dcol_ref,
                    kv_s, kv_sem, kv_flag, s_ref, mx_ref, l_ref, acc_ref):
    t = pl.program_id(0)
    bounds = [sc_ref[1 + d] for d in range(4)]
    hd = acc_ref.shape[1]
    c2 = scale * math.log2(math.e)
    kv = Loader(kv_s, kv_sem, kv_flag)

    @pl.when(t == 0)
    def _():
        start_kv(sc_ref, n_dev, bounds, kv_hbm, kv)

    piece = jnp.where(t == 0, sc_ref[0], 2 * n_dev - 1 - sc_ref[0])
    kt0, kt1 = key_range(bounds, piece)
    mx_ref[...] = jnp.full(mx_ref.shape, NEG_BIG, F32)

    @pl.loop(kt0, kt1)
    def _(kt):
        kv.need(kv_hbm.at[kt], kt)

        def tile(masked):
            s = dot(stack_heads(q_ref[0], 0, hd), kv_s[kt, :, :hd], NT) * c2
            if masked:
                rpos, kpos = row_pos(piece * PIECE, 0), key_pos(kt * PIECE, 1)
                s = jnp.where((kpos <= rpos) & (kpos >= doc_start(bounds, rpos)), s, NEG_BIG)
            s_ref[kt] = s
            mx_ref[...] = fold_lanes(jnp.maximum, mx_ref[...], s)

        masked_or_not(bounds, piece, kt, tile)

    m = jnp.max(mx_ref[...], axis=1, keepdims=True)
    l_ref[...] = jnp.zeros(l_ref.shape, F32)
    acc_ref[...] = jnp.zeros(acc_ref.shape, F32)

    @pl.loop(kt0, kt1)
    def _(kt):
        p = jnp.exp2(s_ref[kt] - m)
        l_ref[...] = fold_lanes(jnp.add, l_ref[...], p)
        acc_ref[...] += dot(p.astype(BF16), kv_s[kt, :, hd:], NN)

    l = jnp.sum(l_ref[...], axis=1, keepdims=True)
    o2 = (acc_ref[...] * (1.0 / l)).astype(BF16)
    o_ref[:, :hd] = o2[:PIECE]
    o_ref[:, hd:] = o2[PIECE:]
    do2 = stack_heads(q_ref[0], 2 * hd, hd)
    delta = jnp.sum(do2.astype(F32) * o2.astype(F32), axis=1, keepdims=True)
    l2 = jnp.broadcast_to(m + jnp.log2(l), (2 * PIECE, LANES))
    delta = jnp.broadcast_to(delta, (2 * PIECE, LANES))
    lcol_ref[0] = l2
    dcol_ref[0] = delta
    ld_ref[0, 0:1] = jnp.transpose(l2)[0:1]
    ld_ref[0, 1:2] = jnp.transpose(delta)[0:1]


def attn_fwd(sc, q, kvg, n_dev, scale):
    n_piece, _, two_hd = kvg.shape
    hd = two_hd // 2
    col = pl.BlockSpec((1, 2 * PIECE, LANES), lambda t, sc: (t, 0, 0))
    col_shape = jax.ShapeDtypeStruct((2, 2 * PIECE, LANES), F32)
    return pl.pallas_call(
        functools.partial(attn_fwd_kernel, n_dev, scale),
        grid_spec=pltpu.PrefetchScalarGridSpec(
            num_scalar_prefetch=1,
            grid=(2,),
            in_specs=[pl.BlockSpec((1, PIECE, 4 * hd), lambda t, sc: (t, 0, 0)), ANY],
            out_specs=[
                pl.BlockSpec((PIECE, two_hd), lambda t, sc: (t, 0)),
                pl.BlockSpec((1, 2, 2 * PIECE), lambda t, sc: (t, 0, 0)),
                col, col,
            ],
            scratch_shapes=[
                *loader_scratch(n_piece, two_hd),
                pltpu.VMEM((n_piece, 2 * PIECE, PIECE), F32),
                pltpu.VMEM((2 * PIECE, LANES), F32),
                pltpu.VMEM((2 * PIECE, LANES), F32),
                pltpu.VMEM((2 * PIECE, hd), F32),
            ],
        ),
        out_shape=[
            jax.ShapeDtypeStruct((2 * PIECE, two_hd), BF16),
            jax.ShapeDtypeStruct((2, 2, 2 * PIECE), F32),
            col_shape, col_shape,
        ],
        compiler_params=pltpu.CompilerParams(vmem_limit_bytes=VMEM_LIMIT, dimension_semantics=("arbitrary",)),
        cost_estimate=pl.CostEstimate(flops=8 * n_piece * PIECE * PIECE * hd, bytes_accessed=kvg.size, transcendentals=0),
        name="attn_fwd",
    )(sc, q, kvg)


def attn_dq_kernel(n_dev, scale, sc_ref, q_ref, lcol_ref, dcol_ref, kv_hbm, dq_ref, kv_s, kv_sem, kv_flag, acc_ref):
    t = pl.program_id(0)
    bounds = [sc_ref[1 + d] for d in range(4)]
    hd = acc_ref.shape[1]
    c2 = scale * math.log2(math.e)
    kv = Loader(kv_s, kv_sem, kv_flag)

    @pl.when(t == 0)
    def _():
        start_kv(sc_ref, n_dev, bounds, kv_hbm, kv)

    piece = jnp.where(t == 0, sc_ref[0], 2 * n_dev - 1 - sc_ref[0])
    kt0, kt1 = key_range(bounds, piece)
    acc_ref[...] = jnp.zeros(acc_ref.shape, F32)

    @pl.loop(kt0, kt1)
    def _(kt):
        kv.need(kv_hbm.at[kt], kt)

        def tile(masked):
            k = kv_s[kt, :, :hd]
            s = dot(stack_heads(q_ref[0], 0, hd), k, NT) * c2 - lcol_ref[0, :, 0:1]
            if masked:
                rpos, kpos = row_pos(piece * PIECE, 0), key_pos(kt * PIECE, 1)
                s = jnp.where((kpos <= rpos) & (kpos >= doc_start(bounds, rpos)), s, NEG_BIG)
            p = jnp.exp2(s).astype(BF16).astype(F32)
            dp = dot(stack_heads(q_ref[0], 2 * hd, hd), kv_s[kt, :, hd:], NT)
            ds = (p * (dp - dcol_ref[0, :, 0:1])).astype(BF16)
            acc_ref[...] += dot(ds, k, NN)

        masked_or_not(bounds, piece, kt, tile)

    dq2 = (acc_ref[...] * scale).astype(BF16)
    dq_ref[:, :hd] = dq2[:PIECE]
    dq_ref[:, hd:] = dq2[PIECE:]


def attn_dq(sc, q, lcol, dcol, kvg, n_dev, scale):
    n_piece, _, two_hd = kvg.shape
    hd = two_hd // 2
    col = pl.BlockSpec((1, 2 * PIECE, LANES), lambda t, sc: (t, 0, 0))
    return pl.pallas_call(
        functools.partial(attn_dq_kernel, n_dev, scale),
        grid_spec=pltpu.PrefetchScalarGridSpec(
            num_scalar_prefetch=1,
            grid=(2,),
            in_specs=[pl.BlockSpec((1, PIECE, 4 * hd), lambda t, sc: (t, 0, 0)), col, col, ANY],
            out_specs=pl.BlockSpec((PIECE, two_hd), lambda t, sc: (t, 0)),
            scratch_shapes=[*loader_scratch(n_piece, two_hd), pltpu.VMEM((2 * PIECE, hd), F32)],
        ),
        out_shape=jax.ShapeDtypeStruct((2 * PIECE, two_hd), BF16),
        compiler_params=pltpu.CompilerParams(vmem_limit_bytes=VMEM_LIMIT, dimension_semantics=("arbitrary",)),
        cost_estimate=pl.CostEstimate(flops=12 * n_piece * PIECE * PIECE * hd, bytes_accessed=kvg.size, transcendentals=0),
        name="attn_dq",
    )(sc, q, lcol, dcol, kvg)


def chips_of(me):
    px, py, _ = neighbours(me)
    chip, core = me // 2, me % 2
    return chip, px // 2, py // 2, px // 2 + py // 2 - chip, core


def attn_kv_kernel(n_dev, scale, own, sc_ref, ld_ref, kv_ref, *refs):
    n_in = 8 if own else 2
    n_out = 1 if own else 3
    qd_in, outs, (qd_s, qd_sem, qd_flag, dk_ref, dv_ref) = refs[:n_in], refs[n_in:n_in + n_out], refs[n_in + n_out:]
    g = pl.program_id(0)
    me = sc_ref[0]
    bounds = [sc_ref[1 + d] for d in range(4)]
    hd = dk_ref.shape[1]
    seq_len = 2 * n_dev * PIECE
    last = 2 * n_dev - 1
    c2 = scale * math.log2(math.e)
    chip, x_chip, y_chip, d_chip, core = chips_of(me)
    par = me + 1 - 2 * core
    qd = Loader(qd_s, qd_sem, qd_flag)

    sources = [(qd_in[0].at[0], me, True), (qd_in[0].at[1], last - me, True), (qd_in[1].at[0], par, True), (qd_in[1].at[1], last - par, True)]
    for same, other, c in zip(qd_in[2::2], qd_in[3::2], (x_chip, y_chip, d_chip)):
        sources.append((same, last - (2 * c + core), c < chip))
        sources.append((other, last - (2 * c + 1 - core), c < chip))

    def end_of(piece):
        return (doc_end(bounds, piece * PIECE + PIECE - 1, seq_len) + PIECE - 1) // PIECE

    @pl.when(g == 0)
    def _():
        for ref, piece, valid in sources:
            if own:
                valid = valid & (((piece >= me) & (piece < end_of(me))) | ((piece >= last - me) & (piece < end_of(last - me))))
            qd.start(ref, piece, valid)

    if own:
        kp = jnp.where(g == 0, me, last - me)
        a0 = jnp.where(g == 0, me, 2 * chip + 2)
        b0 = jnp.where(g == 0, last - 1 - 2 * chip, last - me)
        b1 = last + 1
        live = True
    else:
        tgt = jnp.where(g == 0, x_chip, jnp.where(g == 1, y_chip, d_chip))
        kp = 2 * tgt + core
        a0 = 2 * chip
        b0 = last - 1 - 2 * chip
        b1 = b0 + 2
        live = tgt < chip
    end = end_of(kp)
    na = jnp.maximum(jnp.minimum(2 * chip + 2, end) - a0, 0)
    nb = jnp.maximum(jnp.minimum(b1, end) - b0, 0)
    dk_ref[...] = jnp.zeros(dk_ref.shape, F32)
    dv_ref[...] = jnp.zeros(dv_ref.shape, F32)

    @pl.loop(0, jnp.where(live, na + nb, 0))
    def _(i):
        qp = jnp.where(i < na, a0 + i, b0 + i - na)
        qd.need(sources[0][0], qp)
        slot = jnp.where(qp < n_dev, 2 * qp, 2 * (last - qp) + 1)

        def tile(masked):
            q = qd_s[qp]
            q2, do2 = stack_heads(q, 0, hd), stack_heads(q, 2 * hd, hd)
            s = dot(kv_ref[0, :, :hd], q2, NT) * c2 - ld_ref[slot, 0:1, :]
            if masked:
                qpos, kpos = row_pos(qp * PIECE, 1), key_pos(kp * PIECE, 0)
                s = jnp.where((kpos <= qpos) & (kpos >= doc_start(bounds, qpos)), s, NEG_BIG)
            p = jnp.exp2(s).astype(BF16)
            dp = dot(kv_ref[0, :, hd:], do2, NT)
            ds = (p.astype(F32) * (dp - ld_ref[slot, 1:2, :])).astype(BF16)
            dv_ref[...] += dot(p, do2, NN)
            dk_ref[...] += dot(ds, q2, NN)

        masked_or_not(bounds, qp, kp, tile)

    def put(ref):
        ref[:, :hd] = dk_ref[...] * scale
        ref[:, hd:] = dv_ref[...]

    if own:
        put(outs[0].at[0])
    else:
        for n in range(3):
            @pl.when(g == n)
            def _():
                put(outs[n])

    @pl.when(g == pl.num_programs(0) - 1)
    def _():
        for ref, piece, _ in sources:
            qd.need(ref, piece)


def attn_kv(own, sc, ld_all, kvg, qds, n_dev, scale):
    n_piece, _, two_hd = kvg.shape
    hd = two_hd // 2
    last = n_piece - 1

    def kv_block(g, sc):
        me = sc[0]
        if own:
            return (jnp.where(g == 0, me, last - me), 0, 0)
        _, x_chip, y_chip, d_chip, core = chips_of(me)
        return (2 * jnp.where(g == 0, x_chip, jnp.where(g == 1, y_chip, d_chip)) + core, 0, 0)

    piece_out = jax.ShapeDtypeStruct((PIECE, two_hd), F32)
    return pl.pallas_call(
        functools.partial(attn_kv_kernel, n_dev, scale, own),
        grid_spec=pltpu.PrefetchScalarGridSpec(
            num_scalar_prefetch=1,
            grid=(2 if own else 3,),
            in_specs=[
                pl.BlockSpec(ld_all.shape, lambda g, sc: (0, 0, 0)),
                pl.BlockSpec((1, PIECE, two_hd), kv_block),
            ] + [ANY] * len(qds),
            out_specs=pl.BlockSpec((1, PIECE, two_hd), lambda g, sc: (g, 0, 0)) if own else
            [pl.BlockSpec((PIECE, two_hd), lambda g, sc: (0, 0))] * 3,
            scratch_shapes=[
                *loader_scratch(n_piece, 4 * hd),
                pltpu.VMEM((PIECE, hd), F32),
                pltpu.VMEM((PIECE, hd), F32),
            ],
        ),
        out_shape=jax.ShapeDtypeStruct((2, PIECE, two_hd), F32) if own else [piece_out] * 3,
        compiler_params=pltpu.CompilerParams(vmem_limit_bytes=VMEM_LIMIT, dimension_semantics=("arbitrary",)),
        cost_estimate=pl.CostEstimate(flops=(16 if own else 6) * n_piece * PIECE * PIECE * hd, bytes_accessed=kvg.size, transcendentals=0),
        name="attn_kv_own" if own else "attn_kv_back",
    )(sc, ld_all, kvg, *qds)


def dx_kernel(dq_ref, own_ref, rx_ref, ry_ref, rd_ref, w_ref, dx_ref, lhs):
    qd = dq_ref.shape[1]

    @pl.when(pl.program_id(0) == 0)
    def _():
        lhs[:, :qd] = dq_ref[...]
        lhs[:PIECE, qd:] = (own_ref[0] + rx_ref[...] + ry_ref[...] + rd_ref[...]).astype(BF16)
        lhs[PIECE:, qd:] = own_ref[1].astype(BF16)

    dx_ref[...] = dot(lhs[...], w_ref[...], NT).astype(BF16)


def dx_proj(dq, own, rx, ry, rd, w):
    rows, qd = dq.shape
    d = w.shape[0]
    full = lambda a: pl.BlockSpec(a.shape, lambda j: (0,) * a.ndim)
    return pl.pallas_call(
        dx_kernel,
        grid=(d // PIECE,),
        in_specs=[full(dq), full(own), full(rx), full(ry), full(rd), pl.BlockSpec((PIECE, 2 * qd), lambda j: (j, 0))],
        out_specs=pl.BlockSpec((rows, PIECE), lambda j: (0, j)),
        out_shape=jax.ShapeDtypeStruct((rows, d), BF16),
        scratch_shapes=[pltpu.VMEM((rows, 2 * qd), BF16)],
        compiler_params=pltpu.CompilerParams(vmem_limit_bytes=VMEM_LIMIT, dimension_semantics=("arbitrary",)),
        cost_estimate=pl.CostEstimate(flops=4 * rows * d * qd, bytes_accessed=4 * rows * d, transcendentals=0),
        name="dx_proj",
    )(dq, own, rx, ry, rd, w)


def solution(mesh):
    n_dev = mesh.shape['cp']
    row_spec = P(('dp', 'cp'))
    full_spec = P()

    def chip_pairs(pairs):
        return [(2 * a + c, 2 * b + c) for a, b in pairs for c in range(2)]

    up_x, up_y, up_d = (chip_pairs(p) for p in (((0, 1), (2, 3)), ((0, 2), (1, 3)), ((0, 3), (1, 2))))

    def back(pairs):
        return [(b, a) for a, b in pairs]

    def swap(pairs):
        return [(b, b + 1 - 2 * (b % 2)) for _, b in pairs]

    def local_layer(x_in, dy_in, doc_id, w_q, w_k, w_v, w_o):
        d_model = x_in.shape[1]
        hd = w_q.shape[2]
        scale = hd ** -0.5
        wo = w_o.reshape(2 * hd, d_model)
        kvg, own_q, par_q, up_q, w, docg = proj_gather(
            x_in, dy_in, doc_id.reshape(8, -1), w_q, w_k.reshape(d_model, hd), w_v.reshape(d_model, hd), wo, n_dev)
        bounds = jnp.sum((docg.reshape(1, -1) < jnp.arange(1, 5, dtype=jnp.int32)[:, None]).astype(jnp.int32), axis=1)
        sc = jnp.concatenate([lax.axis_index('cp').astype(jnp.int32)[None], bounds])
        o, ld, lcol, dcol = attn_fwd(sc, own_q, kvg, n_dev, scale)
        ld_all = ld_gather(ld, n_dev).reshape(-1, ld.shape[1], ld.shape[2])
        up_q, ld_all = lax.optimization_barrier((up_q, ld_all))
        ups = []
        for pairs in (up_x, up_y, up_d):
            a = lax.ppermute(up_q, 'cp', pairs)
            ups += [a, lax.ppermute(a, 'cp', swap(pairs))]
        rets = attn_kv(False, sc, ld_all, kvg, (own_q, par_q), n_dev, scale)
        rx, ry, rd = (lax.ppermute(ret, 'cp', back(pairs)) for ret, pairs in zip(rets, (up_x, up_y, up_d)))
        dq = attn_dq(sc, own_q, lcol, dcol, kvg, n_dev, scale)
        y_out = dot(o, wo, NN).astype(BF16)
        dkv = attn_kv(True, sc, ld_all, kvg, (own_q, par_q, *ups), n_dev, scale)
        dx = dx_proj(dq, dkv, rx, ry, rd, w)
        return y_out, dx

    return jax.shard_map(local_layer, mesh=mesh,
                         in_specs=(row_spec, row_spec, row_spec, full_spec, full_spec, full_spec, full_spec),
                         out_specs=(row_spec, row_spec), check_vma=False)
```

```python
import functools
import math

import jax
import jax.numpy as jnp
from jax import lax
from jax.experimental import pallas as pl
from jax.experimental.pallas import tpu as pltpu
from jax.sharding import PartitionSpec as P


NEG_BIG = -1.0e30
BF16 = jnp.bfloat16
F32 = jnp.float32
PIECE = 512
ROWS = 256
LANES = 128
NT = (((1,), (1,)), ((), ()))
NN = (((1,), (0,)), ((), ()))
VMEM_LIMIT = 60 * 1024 * 1024
MESH = pl.DeviceIdType.MESH
ANY = pl.BlockSpec(memory_space=pl.ANY)
VMEM = pl.BlockSpec(memory_space=pltpu.VMEM)


def dot(a, b, dims):
    return lax.dot_general(a, b, dims, preferred_element_type=F32)


def doc_start(bounds, pos):
    out = jnp.zeros_like(pos)
    for b in bounds:
        out = jnp.maximum(out, jnp.where(b <= pos, b, 0))
    return out


def doc_end(bounds, pos, seq_len):
    out = seq_len
    for b in bounds:
        out = jnp.minimum(out, jnp.where(b > pos, b, seq_len))
    return out


def neighbours(me):
    return me + 2 - 4 * ((me // 2) % 2), me + 4 - 8 * (me // 4), me + 1 - 2 * (me % 2)


def entry_barrier(me, n_dev):
    barrier = pltpu.get_barrier_semaphore()
    for d in range(1, n_dev):
        pl.semaphore_signal(barrier, inc=1, device_id={'cp': lax.rem(me + d, n_dev)}, device_id_type=MESH)
    pl.semaphore_wait(barrier, n_dev - 1)


def broadcast_copies(me, n_dev, src, dst, send_sem, recv_sem):
    return [
        pltpu.make_async_remote_copy(
            src_ref=src, dst_ref=dst.at[me], send_sem=send_sem.at[d - 1], recv_sem=recv_sem.at[d - 1],
            device_id={'cp': lax.rem(me + d, n_dev)}, device_id_type=MESH)
        for d in range(1, n_dev)
    ]


def proj_gather_kernel(n_dev, x_hbm, dy_hbm, doc_ref, wq_hbm, wk_hbm, wv_hbm, wo_hbm,
                       kvg, own_hbm, par_hbm, up_hbm, w_hbm, sc_ref,
                       x_s, dy_s, wq_s, w_s, wo_s, kv_s, qd_s, docg_ref,
                       w_sem, x_sem, dy_sem, send_sem, recv_sem, qsend_sem, qrecv_sem, loc_sem, dsend_sem, drecv_sem):
    me = lax.axis_index('cp')
    px, py, pc = neighbours(me)
    pd = px + py - me
    last = 2 * n_dev - 1
    hd = wq_s.shape[2]
    qd = 2 * hd
    tiles = PIECE // ROWS

    w_copies = [pltpu.make_async_copy(a, b, w_sem.at[n]) for n, (a, b) in enumerate(
        ((wk_hbm, w_s.at[:, pl.ds(qd, hd)]), (wv_hbm, w_s.at[:, pl.ds(qd + hd, hd)]), (wq_hbm, wq_s), (wo_hbm, wo_s)))]

    def row_copy(src, dst, sem, tile):
        rows = pl.ds(pl.multiple_of(tile * ROWS, ROWS), ROWS)
        return pltpu.make_async_copy(src.at[rows], dst.at[rows], sem.at[tile])

    w_copies[0].start()
    w_copies[1].start()
    for t in range(2 * tiles):
        row_copy(x_hbm, x_s, x_sem, t).start()
    w_copies[2].start()
    w_copies[3].start()
    for t in range(2 * tiles):
        row_copy(dy_hbm, dy_s, dy_sem, t).start()

    entry_barrier(me, n_dev)
    docg_ref[me] = doc_ref[...]
    doc_copies = broadcast_copies(me, n_dev, doc_ref, docg_ref, dsend_sem, drecv_sem)
    for cp in doc_copies:
        cp.start()

    hops = (
        (kv_s.at[0], me, px), (kv_s.at[1], last - me, px),
        (kv_s.at[0], me, py), (kv_s.at[1], last - me, py),
        (kv_s.at[0], me, pc), (kv_s.at[1], last - me, pc),
        (kvg.at[px], px, py), (kvg.at[last - py], last - py, px),
        (kvg.at[px], px, pc), (kvg.at[last - px], last - px, pc),
        (kvg.at[py], py, pc), (kvg.at[last - py], last - py, pc),
        (kvg.at[pd], pd, pc), (kvg.at[last - pd], last - pd, pc),
    )
    copies = [
        pltpu.make_async_remote_copy(
            src_ref=src, dst_ref=kvg.at[piece], send_sem=send_sem.at[n], recv_sem=recv_sem.at[n],
            device_id={'cp': peer}, device_id_type=MESH)
        for n, (src, piece, peer) in enumerate(hops)
    ]
    local = [pltpu.make_async_copy(src, dst, loc_sem.at[n]) for n, (src, dst) in enumerate((
        (kv_s.at[0], kvg.at[me]), (kv_s.at[1], kvg.at[last - me]), (qd_s.at[0], own_hbm.at[0]), (qd_s.at[1], own_hbm.at[1]), (qd_s.at[1], up_hbm), (w_s, w_hbm)))]
    q_copies = [
        pltpu.make_async_remote_copy(
            src_ref=qd_s.at[n], dst_ref=par_hbm.at[n], send_sem=qsend_sem.at[n], recv_sem=qrecv_sem.at[n],
            device_id={'cp': pc}, device_id_type=MESH)
        for n in range(2)
    ]

    def kv_piece(p):
        @pl.loop(0, tiles)
        def _(h):
            row_copy(x_hbm, x_s, x_sem, p * tiles + h).wait()
            rows = pl.ds(pl.multiple_of(p * PIECE + h * ROWS, ROWS), ROWS)
            out = pl.ds(pl.multiple_of(h * ROWS, ROWS), ROWS)
            kv_s[p, out, :] = dot(x_s[rows, :], w_s[:, qd:], NN).astype(BF16)

    def qd_piece(p):
        @pl.loop(0, tiles)
        def _(h):
            rows = pl.ds(pl.multiple_of(p * PIECE + h * ROWS, ROWS), ROWS)
            out = pl.ds(pl.multiple_of(h * ROWS, ROWS), ROWS)
            qd_s[p, out, 0:qd] = dot(x_s[rows, :], w_s[:, :qd], NN).astype(BF16)
            row_copy(dy_hbm, dy_s, dy_sem, p * tiles + h).wait()
            qd_s[p, out, qd:] = dot(dy_s[rows, :], wo_s[...], NT).astype(BF16)

    w_copies[0].wait()
    w_copies[1].wait()
    kv_piece(0)
    copies[0].start()
    copies[4].start()
    local[0].start()
    kv_piece(1)
    for n in (3, 1, 2, 5):
        copies[n].start()
    local[1].start()
    w_copies[2].wait()

    @pl.loop(0, wq_s.shape[0] // PIECE)
    def _(n):
        rows = pl.ds(pl.multiple_of(n * PIECE, PIECE), PIECE)
        w_s[rows, 0:hd] = wq_s[rows, 0, :]
        w_s[rows, hd:qd] = wq_s[rows, 1, :]

    w_copies[3].wait()
    qd_piece(0)
    q_copies[0].start()
    local[2].start()
    qd_piece(1)
    q_copies[1].start()
    for n in (3, 4, 5):
        local[n].start()
    for arrived, forwards in ((0, (6, 8)), (3, (7, 11)), (1, (9,)), (2, (10,)), (6, (12,)), (7, (13,))):
        copies[arrived].wait_recv()
        for n in forwards:
            copies[n].start()
    for n in (4, 5, 8, 9, 10, 11, 12, 13):
        copies[n].wait_recv()
    for cp in copies:
        cp.wait_send()
    for cp in local + q_copies + doc_copies:
        cp.wait()
    docs = docg_ref[...]
    sc_ref[0] = me
    for d in range(1, 5):
        sc_ref[d] = jnp.sum((docs < d).astype(jnp.int32))


def proj_gather(x, dy, doc, wq, wk, wv, wo, n_dev):
    rows, d = x.shape
    hd = wk.shape[1]
    qd_shape = jax.ShapeDtypeStruct((2, PIECE, 4 * hd), BF16)
    dma = pltpu.SemaphoreType.DMA
    n_tile = rows // ROWS
    return pl.pallas_call(
        functools.partial(proj_gather_kernel, n_dev),
        in_specs=[ANY, ANY, VMEM, ANY, ANY, ANY, ANY],
        out_specs=[ANY] * 5 + [pl.BlockSpec(memory_space=pltpu.SMEM)],
        out_shape=[
            jax.ShapeDtypeStruct((2 * n_dev, PIECE, 2 * hd), BF16),
            qd_shape, qd_shape, jax.ShapeDtypeStruct((PIECE, 4 * hd), BF16),
            jax.ShapeDtypeStruct((d, 4 * hd), BF16),
            jax.ShapeDtypeStruct((5,), jnp.int32),
        ],
        scratch_shapes=[
            pltpu.VMEM((rows, d), BF16), pltpu.VMEM((rows, d), BF16),
            pltpu.VMEM(wq.shape, BF16), pltpu.VMEM((d, 4 * hd), BF16), pltpu.VMEM((2 * hd, d), BF16),
            pltpu.VMEM((2, PIECE, 2 * hd), BF16), pltpu.VMEM((2, PIECE, 4 * hd), BF16), pltpu.VMEM((n_dev,) + doc.shape, jnp.int32),
            *(dma((n,)) for n in (4, n_tile, n_tile, 14, 14, 2, 2, 6, n_dev - 1, n_dev - 1)),
        ],
        compiler_params=pltpu.CompilerParams(vmem_limit_bytes=VMEM_LIMIT, collective_id=0, has_side_effects=True),
        cost_estimate=pl.CostEstimate(flops=12 * rows * d * hd, bytes_accessed=8 * rows * d, transcendentals=0),
        name="proj_gather",
    )(x, dy, doc, wq, wk, wv, wo)


def ld_gather_kernel(n_dev, ld_ref, out_ref, send_sem, recv_sem):
    me = lax.axis_index('cp')
    entry_barrier(me, n_dev)
    out_ref[me] = ld_ref[...]
    copies = broadcast_copies(me, n_dev, ld_ref, out_ref, send_sem, recv_sem)
    for cp in copies:
        cp.start()
    for cp in copies:
        cp.wait()


def ld_gather(ld, n_dev):
    return pl.pallas_call(
        functools.partial(ld_gather_kernel, n_dev),
        in_specs=[VMEM], out_specs=VMEM,
        out_shape=jax.ShapeDtypeStruct((n_dev,) + ld.shape, F32),
        scratch_shapes=[pltpu.SemaphoreType.DMA((n_dev - 1,)), pltpu.SemaphoreType.DMA((n_dev - 1,))],
        compiler_params=pltpu.CompilerParams(collective_id=1, has_side_effects=True),
        cost_estimate=pl.CostEstimate(flops=10_000_000, bytes_accessed=1 << 20, transcendentals=0),
        name="ld_gather",
    )(ld)


class Loader:
    def __init__(self, dst, sem, flag):
        self.dst, self.sem, self.flag = dst, sem, flag

    def copy(self, src, piece):
        return pltpu.make_async_copy(src, self.dst.at[piece], self.sem.at[piece])

    def start(self, src, piece, want):
        self.flag[piece] = jnp.where(want, 1, 0)

        @pl.when(self.flag[piece] == 1)
        def _():
            self.copy(src, piece).start()

    def need(self, src, piece):
        @pl.when(self.flag[piece] == 1)
        def _():
            self.copy(src, piece).wait()
            self.flag[piece] = 0


def loader_scratch(n_piece, width):
    return [pltpu.VMEM((n_piece, PIECE, width), BF16), pltpu.SemaphoreType.DMA((n_piece,)), pltpu.SMEM((n_piece,), jnp.int32)]


def key_range(bounds, piece):
    return doc_start(bounds, piece * PIECE) // PIECE, piece + 1


def start_kv(sc_ref, n_dev, bounds, kv_hbm, kv):
    me = sc_ref[0]
    late = 2 * n_dev - 1 - me
    lo_e, lo_l = key_range(bounds, me)[0], key_range(bounds, late)[0]
    for p in range(2 * n_dev):
        kv.start(kv_hbm.at[p], p, ((p >= lo_e) & (p <= me)) | ((p >= lo_l) & (p <= late)))


def fold_lanes(op, acc, s):
    for j in range(s.shape[1] // LANES):
        acc = op(acc, s[:, j * LANES:(j + 1) * LANES])
    return acc


def stack_heads(a, lo, hd):
    return jnp.concatenate([a[:, lo:lo + hd], a[:, lo + hd:lo + 2 * hd]], axis=0)


def fill_starts(bounds, piece, ref):
    ref[...] = doc_start(bounds, piece * PIECE + lax.broadcasted_iota(jnp.int32, ref.shape, 0) % PIECE)


def mask_rows(s, starts, q_first, k_first):
    rpos = q_first + lax.broadcasted_iota(jnp.int32, starts.shape, 0) % PIECE
    lane = k_first + lax.broadcasted_iota(jnp.int32, (1, LANES), 1)
    parts = []
    for j in range(s.shape[1] // LANES):
        kpos = lane + j * LANES
        parts.append(jnp.where((kpos <= rpos) & (kpos >= starts), s[:, j * LANES:(j + 1) * LANES], NEG_BIG))
    return jnp.concatenate(parts, axis=1)


def masked_or_not(bounds, q_piece, k_piece, body):
    whole = (k_piece < q_piece) & (doc_start(bounds, q_piece * PIECE + PIECE - 1) <= k_piece * PIECE)

    @pl.when(whole)
    def _():
        body(False)

    @pl.when(jnp.logical_not(whole))
    def _():
        body(True)


def attn_fwd_kernel(n_dev, scale, sc_ref, q_ref, kv_hbm, o_ref, ld_ref, lcol_ref, dcol_ref,
                    kv_s, kv_sem, kv_flag, s_ref, mx_ref, l_ref, acc_ref, st_ref):
    t = pl.program_id(0)
    bounds = [sc_ref[1 + d] for d in range(4)]
    hd = acc_ref.shape[1]
    c2 = scale * math.log2(math.e)
    kv = Loader(kv_s, kv_sem, kv_flag)

    @pl.when(t == 0)
    def _():
        start_kv(sc_ref, n_dev, bounds, kv_hbm, kv)

    piece = jnp.where(t == 0, sc_ref[0], 2 * n_dev - 1 - sc_ref[0])
    kt0, kt1 = key_range(bounds, piece)
    fill_starts(bounds, piece, st_ref)
    mx_ref[...] = jnp.full(mx_ref.shape, NEG_BIG, F32)

    @pl.loop(kt0, kt1)
    def _(kt):
        kv.need(kv_hbm.at[kt], kt)

        def tile(masked):
            s = dot(stack_heads(q_ref[0], 0, hd), kv_s[kt, :, :hd], NT) * c2
            if masked:
                s = mask_rows(s, st_ref[...], piece * PIECE, kt * PIECE)
            s_ref[kt] = s
            mx_ref[...] = fold_lanes(jnp.maximum, mx_ref[...], s)

        masked_or_not(bounds, piece, kt, tile)

    m = jnp.max(mx_ref[...], axis=1, keepdims=True)
    l_ref[...] = jnp.zeros(l_ref.shape, F32)
    acc_ref[...] = jnp.zeros(acc_ref.shape, F32)

    @pl.loop(kt0, kt1)
    def _(kt):
        p = jnp.exp2(s_ref[kt] - m)
        l_ref[...] = fold_lanes(jnp.add, l_ref[...], p)
        acc_ref[...] += dot(p.astype(BF16), kv_s[kt, :, hd:], NN)

    l = jnp.sum(l_ref[...], axis=1, keepdims=True)
    o2 = (acc_ref[...] * (1.0 / l)).astype(BF16)
    o_ref[:, :hd] = o2[:PIECE]
    o_ref[:, hd:] = o2[PIECE:]
    do2 = stack_heads(q_ref[0], 2 * hd, hd)
    delta = jnp.sum(do2.astype(F32) * o2.astype(F32), axis=1, keepdims=True)
    l2 = jnp.broadcast_to(m + jnp.log2(l), (2 * PIECE, LANES))
    delta = jnp.broadcast_to(delta, (2 * PIECE, LANES))
    lcol_ref[0] = l2
    dcol_ref[0] = delta
    ld_ref[0, 0:1] = jnp.transpose(l2)[0:1]
    ld_ref[0, 1:2] = jnp.transpose(delta)[0:1]


def attn_fwd(sc, q, kvg, n_dev, scale):
    n_piece, _, two_hd = kvg.shape
    hd = two_hd // 2
    col = pl.BlockSpec((1, 2 * PIECE, LANES), lambda t, sc: (t, 0, 0))
    col_shape = jax.ShapeDtypeStruct((2, 2 * PIECE, LANES), F32)
    return pl.pallas_call(
        functools.partial(attn_fwd_kernel, n_dev, scale),
        grid_spec=pltpu.PrefetchScalarGridSpec(
            num_scalar_prefetch=1,
            grid=(2,),
            in_specs=[pl.BlockSpec((1, PIECE, 4 * hd), lambda t, sc: (t, 0, 0)), ANY],
            out_specs=[
                pl.BlockSpec((PIECE, two_hd), lambda t, sc: (t, 0)),
                pl.BlockSpec((1, 2, 2 * PIECE), lambda t, sc: (t, 0, 0)),
                col, col,
            ],
            scratch_shapes=[
                *loader_scratch(n_piece, two_hd),
                pltpu.VMEM((n_piece, 2 * PIECE, PIECE), F32),
                pltpu.VMEM((2 * PIECE, LANES), F32),
                pltpu.VMEM((2 * PIECE, LANES), F32),
                pltpu.VMEM((2 * PIECE, hd), F32),
                pltpu.VMEM((2 * PIECE, LANES), jnp.int32),
            ],
        ),
        out_shape=[
            jax.ShapeDtypeStruct((2 * PIECE, two_hd), BF16),
            jax.ShapeDtypeStruct((2, 2, 2 * PIECE), F32),
            col_shape, col_shape,
        ],
        compiler_params=pltpu.CompilerParams(vmem_limit_bytes=VMEM_LIMIT, dimension_semantics=("arbitrary",)),
        cost_estimate=pl.CostEstimate(flops=8 * n_piece * PIECE * PIECE * hd, bytes_accessed=kvg.size, transcendentals=0),
        name="attn_fwd",
    )(sc, q, kvg)


def attn_dq_kernel(n_dev, scale, sc_ref, q_ref, lcol_ref, dcol_ref, kv_hbm, dq_ref, kv_s, kv_sem, kv_flag, acc_ref, st_ref):
    t = pl.program_id(0)
    bounds = [sc_ref[1 + d] for d in range(4)]
    hd = acc_ref.shape[1]
    c2 = scale * math.log2(math.e)
    kv = Loader(kv_s, kv_sem, kv_flag)

    @pl.when(t == 0)
    def _():
        start_kv(sc_ref, n_dev, bounds, kv_hbm, kv)

    piece = jnp.where(t == 0, sc_ref[0], 2 * n_dev - 1 - sc_ref[0])
    kt0, kt1 = key_range(bounds, piece)
    fill_starts(bounds, piece, st_ref)
    acc_ref[...] = jnp.zeros(acc_ref.shape, F32)

    @pl.loop(kt0, kt1)
    def _(kt):
        kv.need(kv_hbm.at[kt], kt)

        def tile(masked):
            k = kv_s[kt, :, :hd]
            s = dot(stack_heads(q_ref[0], 0, hd), k, NT) * c2 - lcol_ref[0, :, 0:1]
            if masked:
                s = mask_rows(s, st_ref[...], piece * PIECE, kt * PIECE)
            p = jnp.exp2(s).astype(BF16).astype(F32)
            dp = dot(stack_heads(q_ref[0], 2 * hd, hd), kv_s[kt, :, hd:], NT)
            ds = (p * (dp - dcol_ref[0, :, 0:1])).astype(BF16)
            acc_ref[...] += dot(ds, k, NN)

        masked_or_not(bounds, piece, kt, tile)

    dq2 = (acc_ref[...] * scale).astype(BF16)
    dq_ref[:, :hd] = dq2[:PIECE]
    dq_ref[:, hd:] = dq2[PIECE:]


def attn_dq(sc, q, lcol, dcol, kvg, n_dev, scale):
    n_piece, _, two_hd = kvg.shape
    hd = two_hd // 2
    col = pl.BlockSpec((1, 2 * PIECE, LANES), lambda t, sc: (t, 0, 0))
    return pl.pallas_call(
        functools.partial(attn_dq_kernel, n_dev, scale),
        grid_spec=pltpu.PrefetchScalarGridSpec(
            num_scalar_prefetch=1,
            grid=(2,),
            in_specs=[pl.BlockSpec((1, PIECE, 4 * hd), lambda t, sc: (t, 0, 0)), col, col, ANY],
            out_specs=pl.BlockSpec((PIECE, two_hd), lambda t, sc: (t, 0)),
            scratch_shapes=[*loader_scratch(n_piece, two_hd), pltpu.VMEM((2 * PIECE, hd), F32), pltpu.VMEM((2 * PIECE, LANES), jnp.int32)],
        ),
        out_shape=jax.ShapeDtypeStruct((2 * PIECE, two_hd), BF16),
        compiler_params=pltpu.CompilerParams(vmem_limit_bytes=VMEM_LIMIT, dimension_semantics=("arbitrary",)),
        cost_estimate=pl.CostEstimate(flops=12 * n_piece * PIECE * PIECE * hd, bytes_accessed=kvg.size, transcendentals=0),
        name="attn_dq",
    )(sc, q, lcol, dcol, kvg)


def chips_of(me):
    px, py, _ = neighbours(me)
    chip, core = me // 2, me % 2
    return chip, px // 2, py // 2, px // 2 + py // 2 - chip, core


def attn_kv_kernel(n_dev, scale, target, sc_ref, ld_ref, kv_ref, *refs):
    own = target is None
    n_in = 8 if own else 2
    qd_in, (out_ref, qd_s, qd_sem, qd_flag, dk_ref, dv_ref) = refs[:n_in], refs[n_in:]
    g = pl.program_id(0)
    me = sc_ref[0]
    bounds = [sc_ref[1 + d] for d in range(4)]
    hd = dk_ref.shape[1]
    seq_len = 2 * n_dev * PIECE
    last = 2 * n_dev - 1
    c2 = scale * math.log2(math.e)
    chip, x_chip, y_chip, d_chip, core = chips_of(me)
    par = me + 1 - 2 * core
    qd = Loader(qd_s, qd_sem, qd_flag)

    sources = [(qd_in[0].at[0], me, True), (qd_in[0].at[1], last - me, True), (qd_in[1].at[0], par, True), (qd_in[1].at[1], last - par, True)]
    for same, other, c in zip(qd_in[2::2], qd_in[3::2], (x_chip, y_chip, d_chip)):
        sources.append((same, last - (2 * c + core), c < chip))
        sources.append((other, last - (2 * c + 1 - core), c < chip))

    def end_of(piece):
        return (doc_end(bounds, piece * PIECE + PIECE - 1, seq_len) + PIECE - 1) // PIECE

    if own:
        kp = jnp.where(g == 0, me, last - me)
        a0 = jnp.where(g == 0, me, 2 * chip + 2)
        b0 = jnp.where(g == 0, last - 1 - 2 * chip, last - me)
        b1 = last + 1
        live = True
    else:
        tgt = (x_chip, y_chip, d_chip)[target]
        kp = 2 * tgt + core
        a0 = 2 * chip
        b0 = last - 1 - 2 * chip
        b1 = b0 + 2
        live = tgt < chip
    end = end_of(kp)

    @pl.when(g == 0)
    def _():
        for ref, piece, valid in sources:
            if not own:
                valid = live & (piece < end)
            else:
                valid = valid & (((piece >= me) & (piece < end_of(me))) | ((piece >= last - me) & (piece < end_of(last - me))))
            qd.start(ref, piece, valid)

    na = jnp.maximum(jnp.minimum(2 * chip + 2, end) - a0, 0)
    nb = jnp.maximum(jnp.minimum(b1, end) - b0, 0)
    dk_ref[...] = jnp.zeros(dk_ref.shape, F32)
    dv_ref[...] = jnp.zeros(dv_ref.shape, F32)

    @pl.loop(0, jnp.where(live, na + nb, 0))
    def _(i):
        qp = jnp.where(i < na, a0 + i, b0 + i - na)
        qd.need(sources[0][0], qp)
        slot = jnp.where(qp < n_dev, 2 * qp, 2 * (last - qp) + 1)

        def tile(masked):
            q = qd_s[qp]
            q2, do2 = stack_heads(q, 0, hd), stack_heads(q, 2 * hd, hd)
            s = dot(kv_ref[0, :, :hd], q2, NT) * c2 - ld_ref[slot, 0:1, :]
            if masked:
                qpos = qp * PIECE + lax.broadcasted_iota(jnp.int32, (1, 2 * PIECE), 1) % PIECE
                kpos = kp * PIECE + lax.broadcasted_iota(jnp.int32, (PIECE, 1), 0)
                s = jnp.where((kpos <= qpos) & (kpos >= doc_start(bounds, qpos)), s, NEG_BIG)
            p = jnp.exp2(s).astype(BF16)
            dp = dot(kv_ref[0, :, hd:], do2, NT)
            ds = (p.astype(F32) * (dp - ld_ref[slot, 1:2, :])).astype(BF16)
            dv_ref[...] += dot(p, do2, NN)
            dk_ref[...] += dot(ds, q2, NN)

        masked_or_not(bounds, qp, kp, tile)

    out_ref[0, :, :hd] = dk_ref[...] * scale
    out_ref[0, :, hd:] = dv_ref[...]

    @pl.when(g == pl.num_programs(0) - 1)
    def _():
        for ref, piece, _ in sources:
            qd.need(ref, piece)


def attn_kv(target, sc, ld_all, kvg, qds, n_dev, scale):
    n_piece, _, two_hd = kvg.shape
    hd = two_hd // 2
    last = n_piece - 1
    own = target is None
    n_key = 2 if own else 1

    def kv_block(g, sc):
        me = sc[0]
        if own:
            return (jnp.where(g == 0, me, last - me), 0, 0)
        _, x_chip, y_chip, d_chip, core = chips_of(me)
        return (2 * (x_chip, y_chip, d_chip)[target] + core, 0, 0)

    return pl.pallas_call(
        functools.partial(attn_kv_kernel, n_dev, scale, target),
        grid_spec=pltpu.PrefetchScalarGridSpec(
            num_scalar_prefetch=1,
            grid=(n_key,),
            in_specs=[
                pl.BlockSpec(ld_all.shape, lambda g, sc: (0, 0, 0)),
                pl.BlockSpec((1, PIECE, two_hd), kv_block),
            ] + [ANY] * len(qds),
            out_specs=pl.BlockSpec((1, PIECE, two_hd), lambda g, sc: (g, 0, 0)),
            scratch_shapes=[
                *loader_scratch(n_piece, 4 * hd),
                pltpu.VMEM((PIECE, hd), F32),
                pltpu.VMEM((PIECE, hd), F32),
            ],
        ),
        out_shape=jax.ShapeDtypeStruct((n_key, PIECE, two_hd), F32),
        compiler_params=pltpu.CompilerParams(vmem_limit_bytes=VMEM_LIMIT, dimension_semantics=("arbitrary",)),
        cost_estimate=pl.CostEstimate(flops=(16 if own else 2) * n_piece * PIECE * PIECE * hd, bytes_accessed=kvg.size, transcendentals=0),
        name="attn_kv_own" if own else "attn_kv_back",
    )(sc, ld_all, kvg, *qds)


def dx_kernel(dq_ref, own_ref, rx_ref, ry_ref, rd_ref, w_hbm, dx_ref, lhs, w_s, w_sem):
    qd = dq_ref.shape[1]
    j = pl.program_id(0)

    def block(n):
        rows = pl.ds(pl.multiple_of(n * PIECE, PIECE), PIECE)
        return pltpu.make_async_copy(w_hbm.at[rows], w_s.at[rows], w_sem.at[n])

    @pl.when(j == 0)
    def _():
        for n in range(w_hbm.shape[0] // PIECE):
            block(n).start()
        lhs[:, :qd] = dq_ref[...]
        lhs[:PIECE, qd:] = (own_ref[0] + rx_ref[0] + ry_ref[0] + rd_ref[0]).astype(BF16)
        lhs[PIECE:, qd:] = own_ref[1].astype(BF16)

    block(j).wait()
    dx_ref[...] = dot(lhs[...], w_s[pl.ds(pl.multiple_of(j * PIECE, PIECE), PIECE), :], NT).astype(BF16)


def dx_proj(dq, own, rx, ry, rd, w):
    rows, qd = dq.shape
    d = w.shape[0]
    full = lambda a: pl.BlockSpec(a.shape, lambda j: (0,) * a.ndim)
    return pl.pallas_call(
        dx_kernel,
        grid=(d // PIECE,),
        in_specs=[full(dq), full(own), full(rx), full(ry), full(rd), ANY],
        out_specs=pl.BlockSpec((rows, PIECE), lambda j: (0, j)),
        out_shape=jax.ShapeDtypeStruct((rows, d), BF16),
        scratch_shapes=[pltpu.VMEM((rows, 2 * qd), BF16), pltpu.VMEM(w.shape, BF16), pltpu.SemaphoreType.DMA((d // PIECE,))],
        compiler_params=pltpu.CompilerParams(vmem_limit_bytes=VMEM_LIMIT, dimension_semantics=("arbitrary",)),
        cost_estimate=pl.CostEstimate(flops=4 * rows * d * qd, bytes_accessed=4 * rows * d, transcendentals=0),
        name="dx_proj",
    )(dq, own, rx, ry, rd, w)


def solution(mesh):
    n_dev = mesh.shape['cp']
    row_spec = P(('dp', 'cp'))
    full_spec = P()

    def chip_pairs(pairs):
        return [(2 * a + c, 2 * b + c) for a, b in pairs for c in range(2)]

    up_x, up_y, up_d = (chip_pairs(p) for p in (((0, 1), (2, 3)), ((0, 2), (1, 3)), ((0, 3), (1, 2))))

    def back(pairs):
        return [(b, a) for a, b in pairs]

    def swap(pairs):
        return [(b, b + 1 - 2 * (b % 2)) for _, b in pairs]

    def local_layer(x_in, dy_in, doc_id, w_q, w_k, w_v, w_o):
        d_model = x_in.shape[1]
        hd = w_q.shape[2]
        scale = hd ** -0.5
        wo = w_o.reshape(2 * hd, d_model)
        kvg, own_q, par_q, up_q, w, sc = proj_gather(
            x_in, dy_in, doc_id.reshape(8, -1), w_q, w_k.reshape(d_model, hd), w_v.reshape(d_model, hd), wo, n_dev)
        o, ld, lcol, dcol = attn_fwd(sc, own_q, kvg, n_dev, scale)
        ld_all = ld_gather(ld, n_dev).reshape(-1, ld.shape[1], ld.shape[2])
        up_q, ld_all = lax.optimization_barrier((up_q, ld_all))
        ups = []
        for pairs in (up_d, up_x, up_y):
            ups.append(lax.ppermute(up_q, 'cp', pairs))
        parts, rets = {}, {}
        for n, pairs in ((2, up_d), (1, up_y), (0, up_x)):
            parts[n] = attn_kv(n, sc, ld_all, kvg, (own_q, par_q), n_dev, scale)
            rets[n] = lax.ppermute(parts[n], 'cp', back(pairs))
        dq = attn_dq(sc, own_q, lcol, dcol, kvg, n_dev, scale)
        y_out = dot(o, wo, NN).astype(BF16)
        dq, y_out, *ups = lax.optimization_barrier((dq, y_out, *ups))
        late_q = []
        for a, pairs in zip((ups[1], ups[2], ups[0]), (up_x, up_y, up_d)):
            late_q += [a, lax.ppermute(a, 'cp', swap(pairs))]
        dkv = attn_kv(None, sc, ld_all, kvg, (own_q, par_q, *late_q), n_dev, scale)
        dx = dx_proj(dq, dkv, rets[0], rets[1], rets[2], w)
        return y_out, dx

    return jax.shard_map(local_layer, mesh=mesh,
                         in_specs=(row_spec, row_spec, row_spec, full_spec, full_spec, full_spec, full_spec),
                         out_specs=(row_spec, row_spec), check_vma=False)
```

```python
import functools
import math

import jax
import jax.numpy as jnp
from jax import lax
from jax.experimental import pallas as pl
from jax.experimental.pallas import tpu as pltpu
from jax.sharding import PartitionSpec as P


NEG_BIG = -1.0e30
BF16 = jnp.bfloat16
F32 = jnp.float32
PIECE = 512
ROWS = 256
LANES = 128
NT = (((1,), (1,)), ((), ()))
NN = (((1,), (0,)), ((), ()))
MIB = 1 << 20
VMEM_LIMIT = 60 * MIB
MESH = pl.DeviceIdType.MESH
ANY = pl.BlockSpec(memory_space=pl.ANY)
VMEM = pl.BlockSpec(memory_space=pltpu.VMEM)


def dot(a, b, dims):
    return lax.dot_general(a, b, dims, preferred_element_type=F32)


def doc_start(bounds, pos):
    out = jnp.zeros_like(pos)
    for b in bounds:
        out = jnp.maximum(out, jnp.where(b <= pos, b, 0))
    return out


def doc_end(bounds, pos, seq_len):
    out = seq_len
    for b in bounds:
        out = jnp.minimum(out, jnp.where(b > pos, b, seq_len))
    return out


def neighbours(me):
    return me + 2 - 4 * ((me // 2) % 2), me + 4 - 8 * (me // 4), me + 1 - 2 * (me % 2)


def entry_barrier(me, n_dev):
    barrier = pltpu.get_barrier_semaphore()
    for d in range(1, n_dev):
        pl.semaphore_signal(barrier, inc=1, device_id={'cp': lax.rem(me + d, n_dev)}, device_id_type=MESH)
    pl.semaphore_wait(barrier, n_dev - 1)


def broadcast_copies(me, n_dev, src, dst, send_sem, recv_sem):
    return [
        pltpu.make_async_remote_copy(
            src_ref=src, dst_ref=dst.at[me], send_sem=send_sem.at[d - 1], recv_sem=recv_sem.at[d - 1],
            device_id={'cp': lax.rem(me + d, n_dev)}, device_id_type=MESH)
        for d in range(1, n_dev)
    ]


def proj_gather_kernel(n_dev, x_hbm, dy_hbm, doc_ref, wq_hbm, wk_hbm, wv_hbm, wo_hbm,
                       kvg, own_hbm, par_hbm, up_hbm, w_hbm, sc_ref,
                       x_s, dy_s, wq_s, w_s, wo_s, kv_s, qd_s, docg_ref,
                       w_sem, x_sem, dy_sem, send_sem, recv_sem, qsend_sem, qrecv_sem, loc_sem, dsend_sem, drecv_sem):
    me = lax.axis_index('cp')
    px, py, pc = neighbours(me)
    pd = px + py - me
    last = 2 * n_dev - 1
    hd = wq_s.shape[2]
    qd = 2 * hd
    tiles = PIECE // ROWS

    w_copies = [pltpu.make_async_copy(a, b, w_sem.at[n]) for n, (a, b) in enumerate(
        ((wk_hbm, w_s.at[:, pl.ds(qd, hd)]), (wv_hbm, w_s.at[:, pl.ds(qd + hd, hd)]), (wq_hbm, wq_s), (wo_hbm, wo_s)))]

    def row_copy(src, dst, sem, tile):
        rows = pl.ds(pl.multiple_of(tile * ROWS, ROWS), ROWS)
        return pltpu.make_async_copy(src.at[rows], dst.at[rows], sem.at[tile])

    w_copies[0].start()
    w_copies[1].start()
    for t in range(2 * tiles):
        row_copy(x_hbm, x_s, x_sem, t).start()
    w_copies[2].start()
    w_copies[3].start()
    for t in range(2 * tiles):
        row_copy(dy_hbm, dy_s, dy_sem, t).start()

    entry_barrier(me, n_dev)
    docg_ref[me] = doc_ref[...]
    doc_copies = broadcast_copies(me, n_dev, doc_ref, docg_ref, dsend_sem, drecv_sem)
    for cp in doc_copies:
        cp.start()

    hops = (
        (kv_s.at[0], me, px), (kv_s.at[1], last - me, px),
        (kv_s.at[0], me, py), (kv_s.at[1], last - me, py),
        (kv_s.at[0], me, pc), (kv_s.at[1], last - me, pc),
        (kvg.at[px], px, py), (kvg.at[last - py], last - py, px),
        (kvg.at[px], px, pc), (kvg.at[last - px], last - px, pc),
        (kvg.at[py], py, pc), (kvg.at[last - py], last - py, pc),
        (kvg.at[pd], pd, pc), (kvg.at[last - pd], last - pd, pc),
    )
    copies = [
        pltpu.make_async_remote_copy(
            src_ref=src, dst_ref=kvg.at[piece], send_sem=send_sem.at[n], recv_sem=recv_sem.at[n],
            device_id={'cp': peer}, device_id_type=MESH)
        for n, (src, piece, peer) in enumerate(hops)
    ]
    local = [pltpu.make_async_copy(src, dst, loc_sem.at[n]) for n, (src, dst) in enumerate((
        (kv_s.at[0], kvg.at[me]), (kv_s.at[1], kvg.at[last - me]), (qd_s.at[0], own_hbm.at[0]), (qd_s.at[1], own_hbm.at[1]), (qd_s.at[1], up_hbm), (w_s, w_hbm)))]
    q_copies = [
        pltpu.make_async_remote_copy(
            src_ref=qd_s.at[n], dst_ref=par_hbm.at[n], send_sem=qsend_sem.at[n], recv_sem=qrecv_sem.at[n],
            device_id={'cp': pc}, device_id_type=MESH)
        for n in range(2)
    ]

    def kv_piece(p):
        @pl.loop(0, tiles)
        def _(h):
            row_copy(x_hbm, x_s, x_sem, p * tiles + h).wait()
            rows = pl.ds(pl.multiple_of(p * PIECE + h * ROWS, ROWS), ROWS)
            out = pl.ds(pl.multiple_of(h * ROWS, ROWS), ROWS)
            kv_s[p, out, :] = dot(x_s[rows, :], w_s[:, qd:], NN).astype(BF16)

    def qd_piece(p):
        @pl.loop(0, tiles)
        def _(h):
            rows = pl.ds(pl.multiple_of(p * PIECE + h * ROWS, ROWS), ROWS)
            out = pl.ds(pl.multiple_of(h * ROWS, ROWS), ROWS)
            qd_s[p, out, 0:qd] = dot(x_s[rows, :], w_s[:, :qd], NN).astype(BF16)
            row_copy(dy_hbm, dy_s, dy_sem, p * tiles + h).wait()
            qd_s[p, out, qd:] = dot(dy_s[rows, :], wo_s[...], NT).astype(BF16)

    w_copies[0].wait()
    w_copies[1].wait()
    kv_piece(0)
    copies[0].start()
    copies[4].start()
    local[0].start()
    kv_piece(1)
    for n in (3, 1, 2, 5):
        copies[n].start()
    local[1].start()
    w_copies[2].wait()

    @pl.loop(0, wq_s.shape[0] // PIECE)
    def _(n):
        rows = pl.ds(pl.multiple_of(n * PIECE, PIECE), PIECE)
        w_s[rows, 0:hd] = wq_s[rows, 0, :]
        w_s[rows, hd:qd] = wq_s[rows, 1, :]

    w_copies[3].wait()
    qd_piece(0)
    q_copies[0].start()
    local[2].start()
    qd_piece(1)
    q_copies[1].start()
    for n in (3, 4, 5):
        local[n].start()
    for arrived, forwards in ((0, (6, 8)), (3, (7, 11)), (1, (9,)), (2, (10,)), (6, (12,)), (7, (13,))):
        copies[arrived].wait_recv()
        for n in forwards:
            copies[n].start()
    for n in (4, 5, 8, 9, 10, 11, 12, 13):
        copies[n].wait_recv()
    for cp in copies:
        cp.wait_send()
    for cp in local + q_copies + doc_copies:
        cp.wait()
    docs = docg_ref[...]
    sc_ref[0] = me
    for d in range(1, 5):
        sc_ref[d] = jnp.sum((docs < d).astype(jnp.int32))


def proj_gather(x, dy, doc, wq, wk, wv, wo, n_dev):
    rows, d = x.shape
    hd = wk.shape[1]
    qd_shape = jax.ShapeDtypeStruct((2, PIECE, 4 * hd), BF16)
    dma = pltpu.SemaphoreType.DMA
    n_tile = rows // ROWS
    return pl.pallas_call(
        functools.partial(proj_gather_kernel, n_dev),
        in_specs=[ANY, ANY, VMEM, ANY, ANY, ANY, ANY],
        out_specs=[ANY] * 5 + [pl.BlockSpec(memory_space=pltpu.SMEM)],
        out_shape=[
            jax.ShapeDtypeStruct((2 * n_dev, PIECE, 2 * hd), BF16),
            qd_shape, qd_shape, jax.ShapeDtypeStruct((PIECE, 4 * hd), BF16),
            jax.ShapeDtypeStruct((d, 4 * hd), BF16),
            jax.ShapeDtypeStruct((5,), jnp.int32),
        ],
        scratch_shapes=[
            pltpu.VMEM((rows, d), BF16), pltpu.VMEM((rows, d), BF16),
            pltpu.VMEM(wq.shape, BF16), pltpu.VMEM((d, 4 * hd), BF16), pltpu.VMEM((2 * hd, d), BF16),
            pltpu.VMEM((2, PIECE, 2 * hd), BF16), pltpu.VMEM((2, PIECE, 4 * hd), BF16), pltpu.VMEM((n_dev,) + doc.shape, jnp.int32),
            *(dma((n,)) for n in (4, n_tile, n_tile, 14, 14, 2, 2, 6, n_dev - 1, n_dev - 1)),
        ],
        compiler_params=pltpu.CompilerParams(vmem_limit_bytes=VMEM_LIMIT, collective_id=0, has_side_effects=True),
        cost_estimate=pl.CostEstimate(flops=12 * rows * d * hd, bytes_accessed=8 * rows * d, transcendentals=0),
        name="proj_gather",
    )(x, dy, doc, wq, wk, wv, wo)


def ld_gather_kernel(n_dev, ld_ref, out_ref, send_sem, recv_sem):
    me = lax.axis_index('cp')
    entry_barrier(me, n_dev)
    out_ref[me] = ld_ref[...]
    copies = broadcast_copies(me, n_dev, ld_ref, out_ref, send_sem, recv_sem)
    for cp in copies:
        cp.start()
    for cp in copies:
        cp.wait()


def ld_gather(ld, n_dev):
    return pl.pallas_call(
        functools.partial(ld_gather_kernel, n_dev),
        in_specs=[VMEM], out_specs=VMEM,
        out_shape=jax.ShapeDtypeStruct((n_dev,) + ld.shape, F32),
        scratch_shapes=[pltpu.SemaphoreType.DMA((n_dev - 1,)), pltpu.SemaphoreType.DMA((n_dev - 1,))],
        compiler_params=pltpu.CompilerParams(collective_id=1, has_side_effects=True),
        cost_estimate=pl.CostEstimate(flops=10_000_000, bytes_accessed=1 << 20, transcendentals=0),
        name="ld_gather",
    )(ld)


class Loader:
    def __init__(self, dst, sem, flag):
        self.dst, self.sem, self.flag = dst, sem, flag

    def copy(self, src, piece):
        return pltpu.make_async_copy(src, self.dst.at[piece], self.sem.at[piece])

    def start(self, src, piece, want):
        self.flag[piece] = jnp.where(want, 1, 0)

        @pl.when(self.flag[piece] == 1)
        def _():
            self.copy(src, piece).start()

    def need(self, src, piece):
        @pl.when(self.flag[piece] == 1)
        def _():
            self.copy(src, piece).wait()
            self.flag[piece] = 0


def loader_scratch(n_piece, width):
    return [pltpu.VMEM((n_piece, PIECE, width), BF16), pltpu.SemaphoreType.DMA((n_piece,)), pltpu.SMEM((n_piece,), jnp.int32)]


def key_range(bounds, piece):
    return doc_start(bounds, piece * PIECE) // PIECE, piece + 1


def start_kv(sc_ref, n_dev, bounds, kv_hbm, kv):
    me = sc_ref[0]
    late = 2 * n_dev - 1 - me
    lo_e, lo_l = key_range(bounds, me)[0], key_range(bounds, late)[0]
    for p in range(2 * n_dev):
        kv.start(kv_hbm.at[p], p, ((p >= lo_e) & (p <= me)) | ((p >= lo_l) & (p <= late)))


def fold_lanes(op, acc, s):
    for j in range(s.shape[1] // LANES):
        acc = op(acc, s[:, j * LANES:(j + 1) * LANES])
    return acc


def stack_heads(a, lo, hd):
    return jnp.concatenate([a[:, lo:lo + hd], a[:, lo + hd:lo + 2 * hd]], axis=0)


def fill_starts(bounds, piece, ref):
    ref[...] = doc_start(bounds, piece * PIECE + lax.broadcasted_iota(jnp.int32, ref.shape, 0) % PIECE)


def mask_rows(s, starts, q_first, k_first):
    rpos = q_first + lax.broadcasted_iota(jnp.int32, starts.shape, 0) % PIECE
    lane = k_first + lax.broadcasted_iota(jnp.int32, (1, LANES), 1)
    parts = []
    for j in range(s.shape[1] // LANES):
        kpos = lane + j * LANES
        parts.append(jnp.where((kpos <= rpos) & (kpos >= starts), s[:, j * LANES:(j + 1) * LANES], NEG_BIG))
    return jnp.concatenate(parts, axis=1)


def masked_or_not(bounds, q_piece, k_piece, body):
    whole = (k_piece < q_piece) & (doc_start(bounds, q_piece * PIECE + PIECE - 1) <= k_piece * PIECE)

    @pl.when(whole)
    def _():
        body(False)

    @pl.when(jnp.logical_not(whole))
    def _():
        body(True)


def attn_fwd_kernel(n_dev, scale, sc_ref, q_ref, kv_hbm, o_ref, ld_ref, lcol_ref, dcol_ref,
                    kv_s, kv_sem, kv_flag, s_ref, mx_ref, l_ref, acc_ref, st_ref):
    t = pl.program_id(0)
    bounds = [sc_ref[1 + d] for d in range(4)]
    hd = acc_ref.shape[1]
    c2 = scale * math.log2(math.e)
    kv = Loader(kv_s, kv_sem, kv_flag)

    @pl.when(t == 0)
    def _():
        start_kv(sc_ref, n_dev, bounds, kv_hbm, kv)

    piece = jnp.where(t == 0, sc_ref[0], 2 * n_dev - 1 - sc_ref[0])
    kt0, kt1 = key_range(bounds, piece)
    fill_starts(bounds, piece, st_ref)
    mx_ref[...] = jnp.full(mx_ref.shape, NEG_BIG, F32)

    @pl.loop(kt0, kt1)
    def _(kt):
        kv.need(kv_hbm.at[kt], kt)

        def tile(masked):
            s = dot(stack_heads(q_ref[0], 0, hd), kv_s[kt, :, :hd], NT) * c2
            if masked:
                s = mask_rows(s, st_ref[...], piece * PIECE, kt * PIECE)
            s_ref[kt] = s
            mx_ref[...] = fold_lanes(jnp.maximum, mx_ref[...], s)

        masked_or_not(bounds, piece, kt, tile)

    m = jnp.max(mx_ref[...], axis=1, keepdims=True)
    l_ref[...] = jnp.zeros(l_ref.shape, F32)
    acc_ref[...] = jnp.zeros(acc_ref.shape, F32)

    @pl.loop(kt0, kt1)
    def _(kt):
        p = jnp.exp2(s_ref[kt] - m)
        l_ref[...] = fold_lanes(jnp.add, l_ref[...], p)
        acc_ref[...] += dot(p.astype(BF16), kv_s[kt, :, hd:], NN)

    l = jnp.sum(l_ref[...], axis=1, keepdims=True)
    o2 = (acc_ref[...] * (1.0 / l)).astype(BF16)
    o_ref[:, :hd] = o2[:PIECE]
    o_ref[:, hd:] = o2[PIECE:]
    do2 = stack_heads(q_ref[0], 2 * hd, hd)
    delta = jnp.sum(do2.astype(F32) * o2.astype(F32), axis=1, keepdims=True)
    l2 = jnp.broadcast_to(m + jnp.log2(l), (2 * PIECE, LANES))
    delta = jnp.broadcast_to(delta, (2 * PIECE, LANES))
    lcol_ref[0] = l2
    dcol_ref[0] = delta
    ld_ref[0, 0:1] = jnp.transpose(l2)[0:1]
    ld_ref[0, 1:2] = jnp.transpose(delta)[0:1]


def attn_fwd(sc, q, kvg, n_dev, scale):
    n_piece, _, two_hd = kvg.shape
    hd = two_hd // 2
    col = pl.BlockSpec((1, 2 * PIECE, LANES), lambda t, sc: (t, 0, 0))
    col_shape = jax.ShapeDtypeStruct((2, 2 * PIECE, LANES), F32)
    return pl.pallas_call(
        functools.partial(attn_fwd_kernel, n_dev, scale),
        grid_spec=pltpu.PrefetchScalarGridSpec(
            num_scalar_prefetch=1,
            grid=(2,),
            in_specs=[pl.BlockSpec((1, PIECE, 4 * hd), lambda t, sc: (t, 0, 0)), ANY],
            out_specs=[
                pl.BlockSpec((PIECE, two_hd), lambda t, sc: (t, 0)),
                pl.BlockSpec((1, 2, 2 * PIECE), lambda t, sc: (t, 0, 0)),
                col, col,
            ],
            scratch_shapes=[
                *loader_scratch(n_piece, two_hd),
                pltpu.VMEM((n_piece, 2 * PIECE, PIECE), F32),
                pltpu.VMEM((2 * PIECE, LANES), F32),
                pltpu.VMEM((2 * PIECE, LANES), F32),
                pltpu.VMEM((2 * PIECE, hd), F32),
                pltpu.VMEM((2 * PIECE, LANES), jnp.int32),
            ],
        ),
        out_shape=[
            jax.ShapeDtypeStruct((2 * PIECE, two_hd), BF16),
            jax.ShapeDtypeStruct((2, 2, 2 * PIECE), F32),
            col_shape, col_shape,
        ],
        compiler_params=pltpu.CompilerParams(vmem_limit_bytes=VMEM_LIMIT, dimension_semantics=("arbitrary",)),
        cost_estimate=pl.CostEstimate(flops=8 * n_piece * PIECE * PIECE * hd, bytes_accessed=kvg.size, transcendentals=0),
        name="attn_fwd",
    )(sc, q, kvg)


def attn_dq_kernel(n_dev, scale, sc_ref, q_ref, lcol_ref, dcol_ref, kv_hbm, dq_ref, kv_s, kv_sem, kv_flag, acc_ref, st_ref):
    t = pl.program_id(0)
    bounds = [sc_ref[1 + d] for d in range(4)]
    hd = acc_ref.shape[1]
    c2 = scale * math.log2(math.e)
    kv = Loader(kv_s, kv_sem, kv_flag)

    @pl.when(t == 0)
    def _():
        start_kv(sc_ref, n_dev, bounds, kv_hbm, kv)

    piece = jnp.where(t == 0, sc_ref[0], 2 * n_dev - 1 - sc_ref[0])
    kt0, kt1 = key_range(bounds, piece)
    fill_starts(bounds, piece, st_ref)
    acc_ref[...] = jnp.zeros(acc_ref.shape, F32)

    @pl.loop(kt0, kt1)
    def _(kt):
        kv.need(kv_hbm.at[kt], kt)

        def tile(masked):
            k = kv_s[kt, :, :hd]
            s = dot(stack_heads(q_ref[0], 0, hd), k, NT) * c2 - lcol_ref[0, :, 0:1]
            if masked:
                s = mask_rows(s, st_ref[...], piece * PIECE, kt * PIECE)
            p = jnp.exp2(s).astype(BF16).astype(F32)
            dp = dot(stack_heads(q_ref[0], 2 * hd, hd), kv_s[kt, :, hd:], NT)
            ds = (p * (dp - dcol_ref[0, :, 0:1])).astype(BF16)
            acc_ref[...] += dot(ds, k, NN)

        masked_or_not(bounds, piece, kt, tile)

    dq2 = (acc_ref[...] * scale).astype(BF16)
    dq_ref[:, :hd] = dq2[:PIECE]
    dq_ref[:, hd:] = dq2[PIECE:]


def attn_dq(sc, q, lcol, dcol, kvg, n_dev, scale):
    n_piece, _, two_hd = kvg.shape
    hd = two_hd // 2
    col = pl.BlockSpec((1, 2 * PIECE, LANES), lambda t, sc: (t, 0, 0))
    return pl.pallas_call(
        functools.partial(attn_dq_kernel, n_dev, scale),
        grid_spec=pltpu.PrefetchScalarGridSpec(
            num_scalar_prefetch=1,
            grid=(2,),
            in_specs=[pl.BlockSpec((1, PIECE, 4 * hd), lambda t, sc: (t, 0, 0)), col, col, ANY],
            out_specs=pl.BlockSpec((PIECE, two_hd), lambda t, sc: (t, 0)),
            scratch_shapes=[*loader_scratch(n_piece, two_hd), pltpu.VMEM((2 * PIECE, hd), F32), pltpu.VMEM((2 * PIECE, LANES), jnp.int32)],
        ),
        out_shape=jax.ShapeDtypeStruct((2 * PIECE, two_hd), BF16),
        compiler_params=pltpu.CompilerParams(vmem_limit_bytes=VMEM_LIMIT, dimension_semantics=("arbitrary",)),
        cost_estimate=pl.CostEstimate(flops=12 * n_piece * PIECE * PIECE * hd, bytes_accessed=kvg.size, transcendentals=0),
        name="attn_dq",
    )(sc, q, lcol, dcol, kvg)


def chips_of(me):
    px, py, _ = neighbours(me)
    chip, core = me // 2, me % 2
    return chip, px // 2, py // 2, px // 2 + py // 2 - chip, core


def attn_kv_kernel(n_dev, scale, target, sc_ref, ld_ref, kv_ref, *refs):
    own = target is None
    n_in = 8 if own else 2
    qd_in, (out_ref, qd_s, qd_sem, qd_flag, dk_ref, dv_ref) = refs[:n_in], refs[n_in:]
    g = pl.program_id(0)
    me = sc_ref[0]
    bounds = [sc_ref[1 + d] for d in range(4)]
    hd = dk_ref.shape[1]
    seq_len = 2 * n_dev * PIECE
    last = 2 * n_dev - 1
    c2 = scale * math.log2(math.e)
    chip, x_chip, y_chip, d_chip, core = chips_of(me)
    par = me + 1 - 2 * core
    qd = Loader(qd_s, qd_sem, qd_flag)

    sources = [(qd_in[0].at[0], me, True), (qd_in[0].at[1], last - me, True), (qd_in[1].at[0], par, True), (qd_in[1].at[1], last - par, True)]
    for same, other, c in zip(qd_in[2::2], qd_in[3::2], (x_chip, y_chip, d_chip)):
        sources.append((same, last - (2 * c + core), c < chip))
        sources.append((other, last - (2 * c + 1 - core), c < chip))

    def end_of(piece):
        return (doc_end(bounds, piece * PIECE + PIECE - 1, seq_len) + PIECE - 1) // PIECE

    if own:
        kp = jnp.where(g == 0, me, last - me)
        a0 = jnp.where(g == 0, me, 2 * chip + 2)
        b0 = jnp.where(g == 0, last - 1 - 2 * chip, last - me)
        b1 = last + 1
        live = True
    else:
        tgt = (x_chip, y_chip, d_chip)[target]
        kp = 2 * tgt + core
        a0 = 2 * chip
        b0 = last - 1 - 2 * chip
        b1 = b0 + 2
        live = tgt < chip
    end = end_of(kp)

    @pl.when(g == 0)
    def _():
        for ref, piece, valid in sources:
            if not own:
                valid = live & (piece < end)
            else:
                valid = valid & (((piece >= me) & (piece < end_of(me))) | ((piece >= last - me) & (piece < end_of(last - me))))
            qd.start(ref, piece, valid)

    na = jnp.maximum(jnp.minimum(2 * chip + 2, end) - a0, 0)
    nb = jnp.maximum(jnp.minimum(b1, end) - b0, 0)
    dk_ref[...] = jnp.zeros(dk_ref.shape, F32)
    dv_ref[...] = jnp.zeros(dv_ref.shape, F32)

    @pl.loop(0, jnp.where(live, na + nb, 0))
    def _(i):
        qp = jnp.where(i < na, a0 + i, b0 + i - na)
        qd.need(sources[0][0], qp)
        slot = jnp.where(qp < n_dev, 2 * qp, 2 * (last - qp) + 1)

        def tile(masked):
            q = qd_s[qp]
            q2, do2 = stack_heads(q, 0, hd), stack_heads(q, 2 * hd, hd)
            s = dot(kv_ref[0, :, :hd], q2, NT) * c2 - ld_ref[slot, 0:1, :]
            if masked:
                qpos = qp * PIECE + lax.broadcasted_iota(jnp.int32, (1, 2 * PIECE), 1) % PIECE
                kpos = kp * PIECE + lax.broadcasted_iota(jnp.int32, (PIECE, 1), 0)
                s = jnp.where((kpos <= qpos) & (kpos >= doc_start(bounds, qpos)), s, NEG_BIG)
            p = jnp.exp2(s).astype(BF16)
            dp = dot(kv_ref[0, :, hd:], do2, NT)
            ds = (p.astype(F32) * (dp - ld_ref[slot, 1:2, :])).astype(BF16)
            dv_ref[...] += dot(p, do2, NN)
            dk_ref[...] += dot(ds, q2, NN)

        masked_or_not(bounds, qp, kp, tile)

    out_ref[0, :, :hd] = dk_ref[...] * scale
    out_ref[0, :, hd:] = dv_ref[...]

    @pl.when(g == pl.num_programs(0) - 1)
    def _():
        for ref, piece, _ in sources:
            qd.need(ref, piece)


def attn_kv(target, sc, ld_all, kvg, qds, n_dev, scale):
    n_piece, _, two_hd = kvg.shape
    hd = two_hd // 2
    last = n_piece - 1
    own = target is None
    n_key = 2 if own else 1

    def kv_block(g, sc):
        me = sc[0]
        if own:
            return (jnp.where(g == 0, me, last - me), 0, 0)
        _, x_chip, y_chip, d_chip, core = chips_of(me)
        return (2 * (x_chip, y_chip, d_chip)[target] + core, 0, 0)

    return pl.pallas_call(
        functools.partial(attn_kv_kernel, n_dev, scale, target),
        grid_spec=pltpu.PrefetchScalarGridSpec(
            num_scalar_prefetch=1,
            grid=(n_key,),
            in_specs=[
                pl.BlockSpec(ld_all.shape, lambda g, sc: (0, 0, 0)),
                pl.BlockSpec((1, PIECE, two_hd), kv_block),
            ] + [ANY] * len(qds),
            out_specs=pl.BlockSpec((1, PIECE, two_hd), lambda g, sc: (g, 0, 0)),
            scratch_shapes=[
                *loader_scratch(n_piece, 4 * hd),
                pltpu.VMEM((PIECE, hd), F32),
                pltpu.VMEM((PIECE, hd), F32),
            ],
        ),
        out_shape=jax.ShapeDtypeStruct((n_key, PIECE, two_hd), F32),
        compiler_params=pltpu.CompilerParams(vmem_limit_bytes=VMEM_LIMIT, dimension_semantics=("arbitrary",)),
        cost_estimate=pl.CostEstimate(flops=(16 if own else 2) * n_piece * PIECE * PIECE * hd, bytes_accessed=kvg.size, transcendentals=0),
        name="attn_kv_own" if own else "attn_kv_back",
    )(sc, ld_all, kvg, *qds)


def dx_kernel(dq_ref, own_ref, rx_ref, ry_ref, rd_ref, w_hbm, dx_ref, lhs, w_s, w_sem):
    qd = dq_ref.shape[1]
    j = pl.program_id(0)

    def block(n):
        rows = pl.ds(pl.multiple_of(n * PIECE, PIECE), PIECE)
        return pltpu.make_async_copy(w_hbm.at[rows], w_s.at[rows], w_sem.at[n])

    @pl.when(j == 0)
    def _():
        for n in range(w_hbm.shape[0] // PIECE):
            block(n).start()
        lhs[:, :qd] = dq_ref[...]
        lhs[:PIECE, qd:] = (own_ref[0] + rx_ref[0] + ry_ref[0] + rd_ref[0]).astype(BF16)
        lhs[PIECE:, qd:] = own_ref[1].astype(BF16)

    block(j).wait()
    dx_ref[...] = dot(lhs[...], w_s[pl.ds(pl.multiple_of(j * PIECE, PIECE), PIECE), :], NT).astype(BF16)


def dx_proj(dq, own, rx, ry, rd, w):
    rows, qd = dq.shape
    d = w.shape[0]
    full = lambda a: pl.BlockSpec(a.shape, lambda j: (0,) * a.ndim)
    return pl.pallas_call(
        dx_kernel,
        grid=(d // PIECE,),
        in_specs=[full(dq), full(own), full(rx), full(ry), full(rd), ANY],
        out_specs=pl.BlockSpec((rows, PIECE), lambda j: (0, j)),
        out_shape=jax.ShapeDtypeStruct((rows, d), BF16),
        scratch_shapes=[pltpu.VMEM((rows, 2 * qd), BF16), pltpu.VMEM(w.shape, BF16), pltpu.SemaphoreType.DMA((d // PIECE,))],
        compiler_params=pltpu.CompilerParams(vmem_limit_bytes=VMEM_LIMIT, dimension_semantics=("arbitrary",)),
        cost_estimate=pl.CostEstimate(flops=4 * rows * d * qd, bytes_accessed=4 * rows * d, transcendentals=0),
        name="dx_proj",
    )(dq, own, rx, ry, rd, w)


def solution(mesh):
    n_dev = mesh.shape['cp']
    row_spec = P(('dp', 'cp'))
    full_spec = P()

    def chip_pairs(pairs):
        return [(2 * a + c, 2 * b + c) for a, b in pairs for c in range(2)]

    up_x, up_y, up_d = (chip_pairs(p) for p in (((0, 1), (2, 3)), ((0, 2), (1, 3)), ((0, 3), (1, 2))))

    def back(pairs):
        return [(b, a) for a, b in pairs]

    def swap(pairs):
        return [(b, b + 1 - 2 * (b % 2)) for _, b in pairs]

    def local_layer(x_in, dy_in, doc_id, w_q, w_k, w_v, w_o):
        d_model = x_in.shape[1]
        hd = w_q.shape[2]
        scale = hd ** -0.5
        wo = w_o.reshape(2 * hd, d_model)
        kvg, own_q, par_q, up_q, w, sc = proj_gather(
            x_in, dy_in, doc_id.reshape(8, -1), w_q, w_k.reshape(d_model, hd), w_v.reshape(d_model, hd), wo, n_dev)
        o, ld, lcol, dcol = attn_fwd(sc, own_q, kvg, n_dev, scale)
        ld_all = ld_gather(ld, n_dev).reshape(-1, ld.shape[1], ld.shape[2])
        up_q, ld_all = lax.optimization_barrier((up_q, ld_all))
        ups = []
        for pairs in (up_d, up_x, up_y):
            ups.append(lax.ppermute(up_q, 'cp', pairs))
        parts, rets = {}, {}
        for n, pairs in ((2, up_d), (1, up_y), (0, up_x)):
            parts[n] = attn_kv(n, sc, ld_all, kvg, (own_q, par_q), n_dev, scale)
            rets[n] = lax.ppermute(parts[n], 'cp', back(pairs))
        dq = attn_dq(sc, own_q, lcol, dcol, kvg, n_dev, scale)
        dq, *ups = lax.optimization_barrier((dq, *ups))
        late_q = []
        for a, pairs in ((ups[1], up_x), (ups[2], up_y), (ups[0], up_d)):
            late_q += [a, lax.ppermute(a, 'cp', swap(pairs))]
        y_out = dot(o, wo, NN).astype(BF16)
        dkv = attn_kv(None, sc, ld_all, kvg, (own_q, par_q, *late_q), n_dev, scale)
        dx = dx_proj(dq, dkv, rets[0], rets[1], rets[2], w)
        return y_out, dx

    return jax.shard_map(local_layer, mesh=mesh,
                         in_specs=(row_spec, row_spec, row_spec, full_spec, full_spec, full_spec, full_spec),
                         out_specs=(row_spec, row_spec), check_vma=False)
```
